256 devices in a mesh: grp: 8 (over y, core), seq: 32 (over z, x).
Axes of the slice: x: 4, y: 4, z: 8, core: 2. Of those that a mesh axis runs over, the one named last changes fastest.
Arguments:
- points: bfloat16 [262144, 256], P(('grp', 'seq')), may hold values from -6 to 6
- hilbert_pos: int32 [2048], P(('grp', 'seq')), may hold values from 0 to 63, as said below
- valid_counts: int32 [2048], P(('grp', 'seq')), may hold values from 32 to 128
- norm_params: float32 [2, 4, 256], replicated, may hold values from 0.5 to 1.5
- qkv_weight: bfloat16 [2, 256, 768], replicated
- out_weight: bfloat16 [2, 256, 256], replicated, may hold values from -0.375 to 0.375
- up_weight: bfloat16 [2, 256, 1024], replicated, may hold values from -0.375 to 0.375
- down_weight: bfloat16 [2, 1024, 256], replicated, may hold values from -0.1875 to 0.1875
Outputs:
- features_out: bfloat16 [262144, 256], P(('grp', 'seq'))
The draws below stay inside these ranges and needn't reach their ends.
Inputs may be any that keep to these rules, and one draw needn't show every extreme that they name: A group is the 8 devices with one index of seq. Within each group, hilbert_pos is a permutation of the group's 8 * 8 positions. The owner of position h is the device of index h // 8 along grp in the same group. Each device sends exactly 1 of its cells to each owner of its group.
All inputs are finite; a program needn't handle non-finite values.
Results may differ from the reference program's by a relative error of at most 0.017.
The reference program's roundings to bfloat16 on the way count: a program that leaves them out, or rounds other values in their place, can miss the bound.
Values may be sent and summed in bfloat16 or wider, within the bound.
A program may use at most 64 MiB of HBM per device.

```python
import jax
import jax.numpy as jnp
from jax import lax

C = 256
HEADS = 16
HID = 1024
HD = 16
CELL = 128
PATCH_CELLS = 8
HALF = 4
LAYERS = 2
CELLS = 2048
POINTS = 262144
N_GRP = 8
N_SEQ = 32


def draw_hilbert_pos(key, part):
    per_owner = PATCH_CELLS // N_GRP

    def group_draw(group_key):
        first_key, second_key = jax.random.split(group_key, 2)
        sends = jax.vmap(lambda k: jax.random.permutation(k, PATCH_CELLS).astype(jnp.int32))(jax.random.split(first_key, N_GRP))
        shuffles = jax.vmap(lambda k: jax.random.permutation(k, PATCH_CELLS).astype(jnp.int32))(jax.random.split(second_key, N_GRP))
        owner_index = sends // per_owner
        arrival = jnp.arange(N_GRP, dtype=jnp.int32)[:, None] * per_owner + sends % per_owner
        return (owner_index * PATCH_CELLS + shuffles[owner_index, arrival]).astype(jnp.int32)
    drawn = jax.vmap(group_draw)(jax.random.split(key, N_SEQ))
    return jnp.transpose(drawn, (1, 0, 2)).reshape(-1).astype(jnp.int32)


def draw_qkv_weight(key, part):
    weights_base = jax.random.normal(key, (LAYERS, C, 3 * C), jnp.float32) * C ** (-0.5)
    return weights_base.astype(jnp.bfloat16)


def place_ends(entries, stream_key, low, high):
    dims = entries.shape
    index_at = [jax.random.randint(jax.random.fold_in(stream_key, axis), (), 0, dims[axis]) for axis in range(len(dims))]
    entries = entries.at[tuple(index_at)].set(low)
    longest = dims.index(max(dims))
    index_at[longest] = (index_at[longest] + 1) % dims[longest]
    return entries.at[tuple(index_at)].set(high)


def block_levels(stream_key, shape, pieces, low, high):
    level, own = 1.0, jax.random.fold_in(stream_key, 6)
    for axis_at, parts in pieces:
        draws = jnp.exp(jax.random.uniform(jax.random.fold_in(own, axis_at), (parts,), jnp.float32, low / len(pieces), high / len(pieces)))
        level = level * jnp.repeat(draws, shape[axis_at] // parts).reshape([-1 if axis == axis_at else 1 for axis in range(len(shape))])
    return level


def gaussian(rng, shape, scale, reach, shards=(), kind=jnp.bfloat16):
    gain = block_levels(rng, shape, shards, -0.22, 0.18) if shards else 1.0
    entries = jax.random.normal(rng, shape, jnp.float32) * scale * gain
    return jnp.minimum(jnp.maximum(entries, -reach), reach).astype(kind)


def setup_inputs(seed: int = 0) -> dict:
    splits = jax.random.split(jax.random.key(seed), 9)
    points = gaussian(splits[0], (POINTS, C), 1.0, 6.0, ((0, 256),))
    hilbert_pos = draw_hilbert_pos(jax.random.fold_in(splits[8], 71), 0)
    valid_counts = place_ends(jax.random.randint(splits[2], (CELLS,), CELL // 4, CELL + 1), jax.random.fold_in(splits[2], 1), CELL // 4, CELL).astype(jnp.int32)
    norm_params = jnp.clip(jax.random.uniform(splits[3], (LAYERS, 4, C), jnp.float32, 0.5, 1.5), 0.5, 1.5)
    qkv_weight = draw_qkv_weight(jax.random.fold_in(splits[8], 71), 0)
    out_weight = gaussian(splits[5], (LAYERS, C, C), C ** -0.5, 0.375)
    up_weight = gaussian(splits[6], (LAYERS, C, HID), C ** -0.5, 0.375)
    down_weight = gaussian(splits[7], (LAYERS, HID, C), HID ** -0.5, 0.1875)
    return {"points": points, "hilbert_pos": hilbert_pos, "valid_counts": valid_counts, "norm_params": norm_params, "qkv_weight": qkv_weight, "out_weight": out_weight, "up_weight": up_weight, "down_weight": down_weight}


def layer_norm(values, gain_row, offset):
    center = lax.optimization_barrier(jnp.mean(values, axis=-1, keepdims=True))
    spread = values - center
    second = lax.optimization_barrier(jnp.mean(spread * spread, axis=-1, keepdims=True))
    return spread * lax.rsqrt(second + 1e-05) * gain_row + offset

def attend_rows(queries, keys_rows, values_rows, key_valid):
    query_count = queries.shape[0]
    key_count = keys_rows.shape[0]
    query_heads = queries.astype(jnp.float32).reshape(query_count, HEADS, HD)
    key_heads = keys_rows.astype(jnp.float32).reshape(key_count, HEADS, HD)
    value_heads = values_rows.astype(jnp.float32).reshape(key_count, HEADS, HD)
    scores = jnp.einsum('qhd,khd->hqk', query_heads, key_heads) * HD ** (-0.5)
    scores = jnp.where(key_valid[None, None, :], scores, -1e+30)
    highest = lax.optimization_barrier(jnp.max(scores, axis=-1, keepdims=True))
    exponent = jnp.exp(scores - highest)
    weights_bf = (exponent / lax.optimization_barrier(jnp.sum(exponent, axis=-1, keepdims=True))).astype(jnp.bfloat16)
    mixture = jnp.einsum('hqk,khd->qhd', weights_bf.astype(jnp.float32), value_heads)
    return mixture.reshape(query_count, C).astype(jnp.bfloat16)

def block_rows(window, valid_rows, first_row, row_count, norm_rows, qkv_layer, out_layer, up_layer, down_layer):
    normed = layer_norm(window.astype(jnp.float32), norm_rows[0], norm_rows[1]).astype(jnp.bfloat16)
    qkv = jnp.dot(normed, qkv_layer, preferred_element_type=jnp.float32).astype(jnp.bfloat16)
    queries = qkv[first_row:first_row + row_count, :C]
    mixture = attend_rows(queries, qkv[:, C:2 * C], qkv[:, 2 * C:], valid_rows)
    own_rows = window[first_row:first_row + row_count].astype(jnp.float32)
    residual = own_rows + jnp.dot(mixture, out_layer, preferred_element_type=jnp.float32)
    residual = lax.optimization_barrier(residual.astype(jnp.bfloat16)).astype(jnp.float32)
    normed_two = layer_norm(residual, norm_rows[2], norm_rows[3]).astype(jnp.bfloat16)
    hidden = jax.nn.gelu(jnp.dot(normed_two, up_layer, preferred_element_type=jnp.float32), approximate=False).astype(jnp.bfloat16)
    return (residual + jnp.dot(hidden, down_layer, preferred_element_type=jnp.float32)).astype(jnp.bfloat16)

def reference(points, hilbert_pos, valid_counts, norm_params, qkv_weight, out_weight, up_weight, down_weight):
    cell_rows = points.reshape(CELLS, CELL * C)
    group_index = jnp.arange(CELLS, dtype=jnp.int32) // PATCH_CELLS % N_SEQ
    target = ((hilbert_pos // PATCH_CELLS * N_SEQ + group_index) * PATCH_CELLS + hilbert_pos % PATCH_CELLS).astype(jnp.int32)
    placed = jnp.zeros_like(cell_rows).at[target].set(cell_rows)
    placed_counts = jnp.zeros((CELLS,), jnp.int32).at[target].set(valid_counts)
    current = placed.reshape(CELLS * CELL, C)
    valid = (jnp.arange(CELL, dtype=jnp.int32)[None, :] < placed_counts[:, None]).reshape(-1)
    patch_rows = PATCH_CELLS * CELL
    patch_count = CELLS // PATCH_CELLS

    def aligned_patch(inputs):
        window, window_valid = inputs
        return block_rows(window, window_valid, 0, patch_rows, norm_params[0], qkv_weight[0], out_weight[0], up_weight[0], down_weight[0])

    def shifted_patch(inputs):
        window, window_valid = inputs
        return block_rows(window, window_valid, 0, patch_rows, norm_params[1], qkv_weight[1], out_weight[1], up_weight[1], down_weight[1])
    current = lax.map(aligned_patch, (current.reshape(patch_count, patch_rows, C), valid.reshape(patch_count, patch_rows))).reshape(-1, C)
    shift_rows = HALF * CELL
    rolled = jnp.roll(current, -shift_rows, axis=0)
    rolled_valid = jnp.roll(valid, -shift_rows)
    rolled = lax.map(shifted_patch, (rolled.reshape(patch_count, patch_rows, C), rolled_valid.reshape(patch_count, patch_rows))).reshape(-1, C)
    current = jnp.roll(rolled, shift_rows, axis=0)
    return jnp.where(valid[:, None], current, jnp.zeros((), jnp.bfloat16))
```

```python
import functools
import math

import jax
import jax.numpy as jnp
from jax import lax
from jax.experimental import pallas as pl
from jax.experimental.pallas import tpu as pltpu
from jax.sharding import PartitionSpec as P

C = 256
HEADS = 16
HD = 16
HID = 1024
CELL = 128
CELLS = 8
ROWS = CELL * CELLS
HALF = ROWS // 2
F32 = jnp.float32
BF16 = jnp.bfloat16
MESH = pl.DeviceIdType.MESH
SCORE_SCALE = HD**-0.5 * math.log2(math.e)
SAFE_EXPONENT = 60.0
SAFE_VALUE = 2.0**40


def norm_rows_of(values, gain, offset):
    center = jnp.mean(values, axis=-1, keepdims=True)
    spread = values - center
    second = jnp.mean(spread * spread, axis=-1, keepdims=True)
    return spread * lax.rsqrt(second + 1e-5) * gain + offset


def nt_dot(a, b):
    return lax.dot_general(a, b, (((1,), (1,)), ((), ())), preferred_element_type=F32)


def nn_dot(a, b):
    return jnp.dot(a, b, preferred_element_type=F32)


def project(rows, gain, offset, w_t, w_k, key_valid, k_ref, v_ref, q_ref, k_at, q_at):
    normed = norm_rows_of(rows.astype(F32), gain, offset).astype(BF16)
    count = rows.shape[0]
    k_ref[pl.ds(k_at, count), :] = nn_dot(normed, w_k).astype(BF16)
    values = nt_dot(w_t[C:, :], normed).astype(BF16)
    v_ref[:, pl.ds(k_at, count)] = jnp.where(key_valid, values, jnp.zeros_like(values))
    if q_at is not None:
        q_ref[:, pl.ds(q_at, count)] = nt_dot(w_t[:C, :], normed).astype(BF16)


def head_of_ones(key_valid, count):
    return jnp.where(jnp.broadcast_to(key_valid, (HD, count)), 1.0, 0.0).astype(BF16)


def attend(windows, k_ref, v_ref, one_ref, q_ref, m_ref, exact, unroll):
    def one_head(head):
        row = pl.multiple_of(head * HD, HD)
        half = head // 8
        for q_lo, q_n, k_lo, k_n in windows:
            lane_head = lax.broadcasted_iota(jnp.int32, (C // 2, q_n), 0) // HD
            queries = q_ref[pl.ds(pl.multiple_of(half * 128, 128), 128), q_lo : q_lo + q_n]
            queries = jnp.where(lane_head == head % 8, queries, jnp.zeros_like(queries))
            keys = k_ref[k_lo : k_lo + k_n, pl.ds(pl.multiple_of(half * 128, 128), 128)]
            scores = nn_dot(keys, queries)
            if exact:
                scores = scores - jnp.max(scores, axis=0, keepdims=True)
            weights = jnp.exp2(scores * SCORE_SCALE).astype(BF16)
            values = jnp.concatenate(
                [v_ref[pl.ds(row, HD), k_lo : k_lo + k_n], one_ref[:, k_lo : k_lo + k_n]], axis=0
            )
            mixed = nn_dot(values, weights)
            m_ref[pl.ds(row, HD), q_lo : q_lo + q_n] = (mixed[:HD] / mixed[HD : HD + 1]).astype(BF16)

    def step(i, carry):
        for u in range(unroll):
            one_head(i * unroll + u)
        return carry

    lax.fori_loop(0, HEADS // unroll, step, 0)


def largest_square(ref, channels_last):
    values = ref[...].astype(F32)
    squares = (values * values).astype(BF16)
    own = (
        lax.broadcasted_iota(jnp.int32, (C, 128), 0) // HD
        == lax.broadcasted_iota(jnp.int32, (C, 128), 1)
    )
    pick = jnp.where(own, 1.0, 0.0).astype(BF16)
    if channels_last:
        sums = nn_dot(squares, pick)
        return jnp.max(sums)
    sums = lax.dot_general(pick, squares, (((0,), (0,)), ((), ())), preferred_element_type=F32)
    return jnp.max(sums)


def attend_any(windows, k_ref, v_ref, one_ref, q_ref, m_ref):
    bound = largest_square(k_ref, True) * largest_square(q_ref, False) * SCORE_SCALE**2
    tallest = jnp.max(jnp.abs(v_ref[...].astype(F32)))
    safe = (bound < (SAFE_EXPONENT * SAFE_EXPONENT)) & (tallest < SAFE_VALUE)

    @pl.when(safe)
    def _():
        attend(windows, k_ref, v_ref, one_ref, q_ref, m_ref, False, 2)

    @pl.when(jnp.logical_not(safe))
    def _():
        attend(windows, k_ref, v_ref, one_ref, q_ref, m_ref, True, 1)


def gelu(values):
    return 0.5 * values * (1.0 + lax.erf(values * (2.0**-0.5)))


def finish(rows, mixture_t, gain, offset, out_w, up_w, down_w):
    residual = rows.astype(F32) + nn_dot(mixture_t.astype(F32).T.astype(BF16), out_w)
    residual = residual.astype(BF16).astype(F32)
    normed = norm_rows_of(residual, gain, offset).astype(BF16)
    hidden = gelu(nn_dot(normed, up_w)).astype(BF16)
    return (residual + nn_dot(hidden, down_w)).astype(BF16)


def lane_valid(count):
    return lax.broadcasted_iota(jnp.int32, (1, CELL), 1) < count


def turned(qkv_ref, w_ref):
    for at, source in ((0, 0), (C, 2 * C)):
        w_ref[at : at + C, :] = qkv_ref[:, source : source + C].astype(F32).T.astype(BF16)


STEP = 256


def first_valid(rows, count):
    index = lax.broadcasted_iota(jnp.int32, (CELL, 1), 0)
    return jnp.where(index < count, rows, rows[0:1, :])


def aligned_kernel(
    meta_ref, x_ref, norm_ref, qkv_ref, out_w, up_w, down_w,
    y_ref, count_ref, w_ref, k_ref, v_ref, one_ref, q_ref, m_ref,
):
    turned(qkv_ref, w_ref)
    gain, offset = norm_ref[0:1, :], norm_ref[1:2, :]

    def take(j, carry):
        at = pl.multiple_of(j * CELL, CELL)
        count = meta_ref[1, j]
        rows = first_valid(x_ref[pl.ds(at, CELL), :].astype(F32), count)
        valid = lane_valid(count)
        project(rows, gain, offset, w_ref[...], qkv_ref[:, C : 2 * C], valid, k_ref, v_ref, q_ref, at, at)
        one_ref[:, pl.ds(at, CELL)] = head_of_ones(valid, CELL)
        count_ref[pl.ds(meta_ref[0, j], 1), :] = jnp.full((1, CELL), count, jnp.int32)
        return carry

    lax.fori_loop(0, CELLS, take, 0)
    attend_any(((0, HALF, 0, ROWS), (HALF, HALF, 0, ROWS)), k_ref, v_ref, one_ref, q_ref, m_ref)

    def give(i, carry):
        at = pl.multiple_of(i * STEP, STEP)
        done = finish(
            x_ref[pl.ds(at, STEP), :], m_ref[:, pl.ds(at, STEP)], norm_ref[2:3, :], norm_ref[3:4, :],
            out_w[...], up_w[...], down_w[...],
        )
        for j in range(STEP // CELL):
            to = pl.multiple_of(meta_ref[0, i * (STEP // CELL) + j] * CELL, CELL)
            y_ref[pl.ds(to, CELL), :] = done[j * CELL : (j + 1) * CELL, :]
        return carry

    lax.fori_loop(0, ROWS // STEP, give, 0)


def shifted_kernel(
    count_ref, before_count_ref, after_count_ref, x_ref, before_ref, after_ref,
    norm_ref, qkv_ref, out_w, up_w, down_w,
    y_ref, w_ref, k_ref, v_ref, one_ref, q_ref, m_ref,
):
    turned(qkv_ref, w_ref)
    gain, offset = norm_ref[0:1, :], norm_ref[1:2, :]

    def take(source, counts, first, k_first, queries):
        def one(j, carry):
            at = pl.multiple_of(j * CELL, CELL)
            count = counts[j + first, 0]
            rows = first_valid(source[pl.ds(at, CELL), :].astype(F32), count)
            valid = lane_valid(count)
            k_at = pl.multiple_of(k_first + at, CELL)
            project(
                rows, gain, offset, w_ref[...], qkv_ref[:, C : 2 * C], valid, k_ref, v_ref, q_ref,
                k_at, at if queries else None,
            )
            one_ref[:, pl.ds(k_at, CELL)] = head_of_ones(valid, CELL)
            return carry

        lax.fori_loop(0, source.shape[0] // CELL, one, 0)

    take(before_ref, before_count_ref, CELLS // 2, 0, False)
    take(x_ref, count_ref, 0, HALF, True)
    take(after_ref, after_count_ref, 0, HALF + ROWS, False)
    attend_any(((0, HALF, 0, ROWS), (HALF, HALF, ROWS, ROWS)), k_ref, v_ref, one_ref, q_ref, m_ref)

    def give(i, carry):
        at = pl.multiple_of(i * STEP, STEP)
        done = finish(
            x_ref[pl.ds(at, STEP), :], m_ref[:, pl.ds(at, STEP)], norm_ref[2:3, :], norm_ref[3:4, :],
            out_w[...], up_w[...], down_w[...],
        )
        for j in range(STEP // CELL):
            index = lax.broadcasted_iota(jnp.int32, (CELL, 1), 0)
            keep = index < count_ref[i * (STEP // CELL) + j, 0]
            part = done[j * CELL : (j + 1) * CELL, :]
            y_ref[pl.ds(pl.multiple_of(at + j * CELL, CELL), CELL), :] = jnp.where(
                keep, part, jnp.zeros_like(part)
            )
        return carry

    lax.fori_loop(0, ROWS // STEP, give, 0)


def vmem():
    return pl.BlockSpec(memory_space=pltpu.VMEM)


def smem():
    return pl.BlockSpec(memory_space=pltpu.SMEM)


def scratch(keys):
    return [
        pltpu.VMEM((2 * C, C), BF16),
        pltpu.VMEM((keys, C), BF16),
        pltpu.VMEM((C, keys), BF16),
        pltpu.VMEM((HD, keys), BF16),
        pltpu.VMEM((C, ROWS), BF16),
        pltpu.VMEM((C, ROWS), BF16),
    ]


def aligned_block(meta, rows, norms, qkv, out_w, up_w, down_w):
    return pl.pallas_call(
        aligned_kernel,
        out_shape=(
            jax.ShapeDtypeStruct((ROWS, C), BF16),
            jax.ShapeDtypeStruct((CELLS, CELL), jnp.int32),
        ),
        in_specs=[smem()] + [vmem()] * 6,
        out_specs=(vmem(), vmem()),
        scratch_shapes=scratch(ROWS),
        compiler_params=pltpu.CompilerParams(vmem_limit_bytes=48 * 2**20),
        name="aligned",
    )(meta, rows, norms, qkv, out_w, up_w, down_w)


def shifted_block(counts, before_counts, after_counts, rows, before, after, norms, qkv, out_w, up_w, down_w):
    return pl.pallas_call(
        shifted_kernel,
        out_shape=jax.ShapeDtypeStruct((ROWS, C), BF16),
        in_specs=[smem()] * 3 + [vmem()] * 8,
        out_specs=vmem(),
        scratch_shapes=scratch(2 * ROWS),
        compiler_params=pltpu.CompilerParams(vmem_limit_bytes=48 * 2**20),
        name="shifted",
    )(counts, before_counts, after_counts, rows, before, after, norms, qkv, out_w, up_w, down_w)


def enter(partners):
    barrier = pltpu.get_barrier_semaphore()
    for partner in partners:
        pl.semaphore_signal(barrier, inc=1, device_id=partner, device_id_type=MESH)
    return lambda: pl.semaphore_wait(barrier, len(partners))


def gather_kernel(pos_ref, count_ref, x_ref, y_ref, meta_ref, out_buf, note_out, note_in, send, recv, note_send, note_recv):
    me, seq = lax.axis_index("grp"), lax.axis_index("seq")
    wait = enter([(lax.rem(me + r, CELLS), seq) for r in range(1, CELLS)])
    for owner in range(CELLS):
        index, place, count = jnp.int32(0), jnp.int32(0), jnp.int32(0)
        for j in range(CELLS):
            position = pos_ref[j]
            mine = position // CELLS == owner
            index = jnp.where(mine, j, index)
            place = jnp.where(mine, position % CELLS, place)
            count = jnp.where(mine, count_ref[j], count)
        out_buf[owner] = x_ref[index]
        row = lax.broadcasted_iota(jnp.int32, (CELLS, CELL), 0)
        note_out[owner] = jnp.where(row == 0, place, count)
    wait()
    copies = []
    for r in range(1, CELLS):
        owner = lax.rem(me + r, CELLS)
        copies.append(pltpu.make_async_remote_copy(
            out_buf.at[owner], y_ref.at[me], send.at[r], recv.at[r], device_id=(owner, seq), device_id_type=MESH))
        copies.append(pltpu.make_async_remote_copy(
            note_out.at[owner], note_in.at[me], note_send.at[r], note_recv.at[r], device_id=(owner, seq), device_id_type=MESH))
    for copy in copies:
        copy.start()
    y_ref[me] = out_buf[me]
    note_in[me] = note_out[me]
    for copy in copies:
        copy.wait()
    lane = lax.broadcasted_iota(jnp.int32, (CELLS, CELL), 1)
    meta = jnp.zeros((CELLS, CELL), jnp.int32)
    for j in range(CELLS):
        meta = jnp.where(lane == j, note_in[j], meta)
    meta_ref[...] = meta


def gather_cells(pos, counts, rows):
    return pl.pallas_call(
        gather_kernel,
        out_shape=(
            jax.ShapeDtypeStruct((CELLS, CELL, C), BF16),
            jax.ShapeDtypeStruct((CELLS, CELL), jnp.int32),
        ),
        in_specs=[smem(), smem(), vmem()],
        out_specs=(vmem(), vmem()),
        scratch_shapes=[
            pltpu.VMEM((CELLS, CELL, C), BF16),
            pltpu.VMEM((CELLS, CELLS, CELL), jnp.int32),
            pltpu.VMEM((CELLS, CELLS, CELL), jnp.int32),
            pltpu.SemaphoreType.DMA((CELLS,)),
            pltpu.SemaphoreType.DMA((CELLS,)),
            pltpu.SemaphoreType.DMA((CELLS,)),
            pltpu.SemaphoreType.DMA((CELLS,)),
        ],
        compiler_params=pltpu.CompilerParams(collective_id=0, has_side_effects=True),
        name="gather_cells",
    )(pos, counts, rows)


def along(step):
    n_grp, n_seq = lax.axis_size("grp"), lax.axis_size("seq")
    flat = lax.axis_index("grp") * n_seq + lax.axis_index("seq")
    other = lax.rem(flat + step + n_grp * n_seq, n_grp * n_seq)
    return (other // n_seq, lax.rem(other, n_seq))


def exchange_kernel(count_ref, x_ref, before_ref, after_ref, before_count_ref, after_count_ref, send, recv):
    after, before = along(1), along(-1)
    enter([after, before])()
    copies = [
        pltpu.make_async_remote_copy(
            source, target, send.at[i], recv.at[i], device_id=device, device_id_type=MESH)
        for i, (source, target, device) in enumerate((
            (x_ref.at[pl.ds(HALF, HALF)], before_ref, after),
            (x_ref.at[pl.ds(0, HALF)], after_ref, before),
            (count_ref, before_count_ref, after),
            (count_ref, after_count_ref, before),
        ))
    ]
    for copy in copies:
        copy.start()
    for copy in copies:
        copy.wait()


def exchange_halves(counts, rows):
    return pl.pallas_call(
        exchange_kernel,
        out_shape=(
            jax.ShapeDtypeStruct((HALF, C), BF16),
            jax.ShapeDtypeStruct((HALF, C), BF16),
            jax.ShapeDtypeStruct((CELLS, CELL), jnp.int32),
            jax.ShapeDtypeStruct((CELLS, CELL), jnp.int32),
        ),
        in_specs=[vmem(), vmem()],
        out_specs=(vmem(),) * 4,
        scratch_shapes=[pltpu.SemaphoreType.DMA((4,)), pltpu.SemaphoreType.DMA((4,))],
        compiler_params=pltpu.CompilerParams(collective_id=1, has_side_effects=True),
        name="exchange_halves",
    )(counts, rows)


def body(points, hilbert_pos, valid_counts, norm_params, qkv_weight, out_weight, up_weight, down_weight):
    placed, meta = gather_cells(hilbert_pos, valid_counts, points.reshape(CELLS, CELL, C))
    aligned, counts = aligned_block(
        meta, placed.reshape(ROWS, C), norm_params[0], qkv_weight[0], out_weight[0], up_weight[0], down_weight[0]
    )
    before, after, before_counts, after_counts = exchange_halves(counts, aligned)
    return shifted_block(
        counts, before_counts, after_counts, aligned, before, after,
        norm_params[1], qkv_weight[1], out_weight[1], up_weight[1], down_weight[1],
    )


def solution(mesh):
    return jax.shard_map(
        body,
        mesh=mesh,
        in_specs=(
            P(("grp", "seq"), None), P(("grp", "seq")), P(("grp", "seq")), P(), P(), P(), P(), P(),
        ),
        out_specs=P(("grp", "seq"), None),
        check_vma=False,
    )
```

```python
import math

import jax
import jax.numpy as jnp
from jax import lax
from jax.experimental import pallas as pl
from jax.experimental.pallas import tpu as pltpu
from jax.sharding import PartitionSpec as P

C = 256
HEADS = 16
HD = 16
HID = 1024
CELL = 128
CELLS = 8
ROWS = CELL * CELLS
HALF = ROWS // 2
STEP = 2 * CELL
F32 = jnp.float32
BF16 = jnp.bfloat16
I32 = jnp.int32
MESH = pl.DeviceIdType.MESH
SCORE_SCALE = HD**-0.5 * math.log2(math.e)
SAFE_EXPONENT = 60.0
SAFE_VALUE = 2.0**40


def nt_dot(a, b):
    return lax.dot_general(a, b, (((1,), (1,)), ((), ())), preferred_element_type=F32)


def nn_dot(a, b):
    return jnp.dot(a, b, preferred_element_type=F32)


def norm_rows_of(values, gain, offset):
    center = jnp.mean(values, axis=-1, keepdims=True)
    spread = values - center
    second = jnp.mean(spread * spread, axis=-1, keepdims=True)
    return spread * lax.rsqrt(second + 1e-5) * gain + offset


def head_pick(rows, columns, channel_axis):
    channel = lax.broadcasted_iota(I32, (rows, columns), channel_axis) // HD
    head = lax.broadcasted_iota(I32, (rows, columns), 1 - channel_axis)
    return jnp.where(channel == head, 1.0, 0.0).astype(BF16)


def first_valid(rows, count):
    index = lax.broadcasted_iota(I32, (CELL, 1), 0)
    return jnp.where(index < count, rows, rows[0:1, :])


def lane_valid(count):
    return jnp.where(lax.broadcasted_iota(I32, (1, CELL), 1) < count, 1.0, 0.0)


def project(rows, valid, gain, offset, w_t, w_k, k_ref, v_ref, q_ref, peak_ref, k_at, q_at):
    count = rows.shape[0]
    normed = norm_rows_of(rows, gain, offset).astype(BF16)
    keys = nn_dot(normed, w_k).astype(BF16)
    k_ref[pl.ds(k_at, count), :] = keys
    values = nt_dot(w_t[C:, :], normed) * valid
    v_ref[:, pl.ds(k_at, count)] = values.astype(BF16)
    wide = keys.astype(F32)
    sums = nn_dot((wide * wide).astype(BF16), head_pick(C, CELL, 0))
    peak_ref[0:1, :] = jnp.maximum(peak_ref[0:1, :], jnp.max(sums, axis=0, keepdims=True))
    tall = jnp.max(jnp.abs(values), axis=0, keepdims=True)
    peak_ref[2:3, :] = jnp.maximum(peak_ref[2:3, :], jnp.maximum(tall[:, :CELL], tall[:, count - CELL :]))
    if q_at is not None:
        queries = nt_dot(w_t[:C, :], normed).astype(BF16)
        q_ref[:, pl.ds(q_at, count)] = queries
        wide = queries.astype(F32)
        sums = nn_dot(head_pick(HEADS, C, 1), (wide * wide).astype(BF16))
        tall = jnp.max(sums, axis=0, keepdims=True)
        peak_ref[1:2, :] = jnp.maximum(peak_ref[1:2, :], jnp.maximum(tall[:, :CELL], tall[:, count - CELL :]))


def turn(qkv_ref, w_ref):
    for at, source in ((0, 0), (C, 2 * C)):
        w_ref[at : at + C, :] = qkv_ref[:, source : source + C].astype(F32).T.astype(BF16)


def attend(windows, pads, k_ref, v_ref, q_ref, m_ref, exact, unroll):
    def one_head(head):
        row = pl.multiple_of(head * HD, HD)
        half = pl.ds(pl.multiple_of((head // 8) * CELL, CELL), CELL)
        for q_lo, q_n, k_lo, k_n in windows:
            lane_head = lax.broadcasted_iota(I32, (CELL, q_n), 0) // HD
            queries = q_ref[half, q_lo : q_lo + q_n]
            queries = jnp.where(lane_head == head % 8, queries, jnp.zeros_like(queries))
            scores = nn_dot(k_ref[k_lo : k_lo + k_n, half], queries)
            if exact:
                scores = scores - jnp.max(scores, axis=0, keepdims=True)
            weights = jnp.exp2(scores * SCORE_SCALE)
            total = jnp.sum(jnp.sum(weights.reshape(k_n // 8, 8, q_n), axis=0), axis=0, keepdims=True)
            for cell in range(k_n // CELL):
                total = total - pads[k_lo // CELL + cell] * weights[cell * CELL : cell * CELL + 1, :]
            mixed = nn_dot(v_ref[pl.ds(row, HD), k_lo : k_lo + k_n], weights.astype(BF16))
            m_ref[pl.ds(row, HD), q_lo : q_lo + q_n] = (mixed / total).astype(BF16)

    def step(i, carry):
        for u in range(unroll):
            one_head(i * unroll + u)
        return carry

    lax.fori_loop(0, HEADS // unroll, step, 0)


def attend_any(windows, pads, peak_ref, k_ref, v_ref, q_ref, m_ref):
    bound = peak_ref[0, 0] * peak_ref[1, 0] * SCORE_SCALE**2
    safe = (bound < SAFE_EXPONENT * SAFE_EXPONENT) & (peak_ref[2, 0] < SAFE_VALUE)

    @pl.when(safe)
    def _():
        attend(windows, pads, k_ref, v_ref, q_ref, m_ref, False, 4)

    @pl.when(jnp.logical_not(safe))
    def _():
        attend(windows, pads, k_ref, v_ref, q_ref, m_ref, True, 1)


def gelu(values):
    return 0.5 * values * (1.0 + lax.erf(values * (2.0**-0.5)))


def finish(rows, mixture_t, gain, offset, out_w, up_w, down_w):
    residual = rows.astype(F32) + nn_dot(mixture_t.astype(F32).T.astype(BF16), out_w)
    residual = residual.astype(BF16).astype(F32)
    normed = norm_rows_of(residual, gain, offset).astype(BF16)
    hidden = gelu(nn_dot(normed, up_w)).astype(BF16)
    return (residual + nn_dot(hidden, down_w)).astype(BF16)


def widest(peak_ref):
    peak_ref[...] = jnp.broadcast_to(jnp.max(peak_ref[...], axis=1, keepdims=True), peak_ref.shape)


def started(*pairs):
    copies = [pltpu.make_async_copy(*pair) for pair in pairs]
    for copy in copies:
        copy.start()
    return copies


def finished(copies):
    for copy in copies:
        copy.wait()


def gather_kernel(
    pos_ref, count_ref, x_hbm, norm_ref, qkv_hbm,
    cells_hbm, k_hbm, v_hbm, q_hbm, meta_ref, peak_ref,
    x_buf, out_buf, in_buf, note_out, note_in, qkv_ref, w_ref, k_ref, v_ref, q_ref,
    load_sem, store_sem, send, recv, note_send, note_recv,
):
    me, seq = lax.axis_index("grp"), lax.axis_index("seq")
    barrier = pltpu.get_barrier_semaphore()
    for r in range(1, CELLS):
        pl.semaphore_signal(barrier, inc=1, device_id=(lax.rem(me + r, CELLS), seq), device_id_type=MESH)
    loads = started((x_hbm, x_buf, load_sem.at[0]), (qkv_hbm.at[0], qkv_ref, load_sem.at[1]))
    finished(loads[:1])
    row = lax.broadcasted_iota(I32, (CELLS, CELL), 0)
    for owner in range(CELLS):
        index, place, count = jnp.int32(0), jnp.int32(0), jnp.int32(0)
        for j in range(CELLS):
            position = pos_ref[j]
            mine = position // CELLS == owner
            index = jnp.where(mine, j, index)
            place = jnp.where(mine, position % CELLS, place)
            count = jnp.where(mine, count_ref[j], count)
        out_buf[owner] = x_buf[index]
        note_out[owner] = jnp.where(row == 0, place, count)
    finished(loads[1:])
    turn(qkv_ref, w_ref)
    pl.semaphore_wait(barrier, CELLS - 1)

    def sent(r):
        owner = lax.rem(me + r, CELLS)
        return (
            pltpu.make_async_remote_copy(
                out_buf.at[owner], in_buf.at[me], send.at[r], recv.at[r],
                device_id=(owner, seq), device_id_type=MESH),
            pltpu.make_async_remote_copy(
                note_out.at[owner], note_in.at[me], note_send.at[r], note_recv.at[r],
                device_id=(owner, seq), device_id_type=MESH),
        )

    copies = [sent(r) for r in range(1, CELLS)]
    for pair in copies:
        for copy in pair:
            copy.start()
    gain, offset = norm_ref[0, 0:1, :], norm_ref[0, 1:2, :]
    peak_ref[...] = jnp.zeros_like(peak_ref)

    def take(j):
        at = pl.multiple_of(j * CELL, CELL)
        count = note_in[j, 1:2, :]
        rows = first_valid(in_buf[j].astype(F32), count[:, 0:1])
        project(
            rows, lane_valid(count), gain, offset, w_ref[...], qkv_ref[:, C : 2 * C],
            k_ref, v_ref, q_ref, peak_ref, at, at,
        )

    def given(r):
        j = lax.rem(me - r + CELLS, CELLS)
        lanes = pl.ds(pl.multiple_of(j * CELL, CELL), CELL)
        return (
            (in_buf.at[j], cells_hbm.at[j], store_sem.at[r, 0]),
            (k_ref.at[lanes, :], k_hbm.at[lanes, :], store_sem.at[r, 1]),
            (v_ref.at[:, lanes], v_hbm.at[:, lanes], store_sem.at[r, 2]),
            (q_ref.at[:, lanes], q_hbm.at[:, lanes], store_sem.at[r, 3]),
        )

    in_buf[me] = out_buf[me]
    note_in[me] = note_out[me]
    take(me)
    started(*given(0))

    def arrive(r, carry):
        for copy in sent(r):
            copy.wait_recv()
        take(lax.rem(me - r + CELLS, CELLS))
        started(*given(r))
        return carry

    lax.fori_loop(1, CELLS, arrive, 0)
    lane = lax.broadcasted_iota(I32, (CELLS, CELL), 1)
    meta = jnp.zeros((CELLS, CELL), I32)
    for j in range(CELLS):
        meta = jnp.where(lane == j, note_in[j], meta)
    meta_ref[...] = meta
    widest(peak_ref)
    for pair in copies:
        for copy in pair:
            copy.wait_send()
    for r in range(CELLS):
        finished([pltpu.make_async_copy(*triple) for triple in given(r)])


def vmem():
    return pl.BlockSpec(memory_space=pltpu.VMEM)


def smem():
    return pl.BlockSpec(memory_space=pltpu.SMEM)


def hbm():
    return pl.BlockSpec(memory_space=pl.ANY)


def shape(dims, dtype=BF16):
    return jax.ShapeDtypeStruct(dims, dtype)


def dma(*dims):
    return pltpu.SemaphoreType.DMA(dims)


def gather_cells(pos, counts, cells, norms, qkv):
    return pl.pallas_call(
        gather_kernel,
        out_shape=(
            shape((CELLS, CELL, C)), shape((ROWS, C)), shape((C, ROWS)), shape((C, ROWS)),
            shape((CELLS, CELL), I32), shape((CELLS, CELL), F32),
        ),
        in_specs=[smem(), smem(), hbm(), vmem(), hbm()],
        out_specs=(hbm(), hbm(), hbm(), hbm(), vmem(), vmem()),
        scratch_shapes=[
            pltpu.VMEM((CELLS, CELL, C), BF16),
            pltpu.VMEM((CELLS, CELL, C), BF16),
            pltpu.VMEM((CELLS, CELL, C), BF16),
            pltpu.VMEM((CELLS, CELLS, CELL), I32),
            pltpu.VMEM((CELLS, CELLS, CELL), I32),
            pltpu.VMEM((C, 3 * C), BF16),
            pltpu.VMEM((2 * C, C), BF16),
            pltpu.VMEM((ROWS, C), BF16),
            pltpu.VMEM((C, ROWS), BF16),
            pltpu.VMEM((C, ROWS), BF16),
            dma(2), dma(CELLS, 4), dma(CELLS), dma(CELLS), dma(CELLS), dma(CELLS),
        ],
        compiler_params=pltpu.CompilerParams(
            collective_id=0, has_side_effects=True, vmem_limit_bytes=24 * 2**20),
        name="gather_cells",
    )(pos, counts, cells, norms, qkv)


def aligned_kernel(
    meta_hbm, peak_hbm, k_hbm, v_hbm, q_hbm, cells_hbm, m_ref, placed_hbm, count_ref,
    meta_ref, peak_ref, k_ref, v_ref, q_ref, sems, place_sems,
):
    loads = started(
        (meta_hbm, meta_ref, sems.at[0]), (peak_hbm, peak_ref, sems.at[1]),
        (k_hbm, k_ref, sems.at[2]), (v_hbm, v_ref, sems.at[3]),
    )
    finished(loads[:1])
    moves, places = [], []
    for j in range(CELLS):
        to = meta_ref[0, j]
        lanes = pl.ds(pl.multiple_of(to * CELL, CELL), CELL)
        moves += started((q_hbm.at[:, pl.ds(j * CELL, CELL)], q_ref.at[:, lanes], place_sems.at[0, j]))
        places += started((cells_hbm.at[j], placed_hbm.at[to], place_sems.at[1, j]))
        count_ref[pl.ds(to, 1), :] = jnp.full((1, CELL), meta_ref[1, j], I32)
    finished(loads[1:])
    finished(moves)
    pads = [(CELL - meta_ref[1, j]).astype(F32) for j in range(CELLS)]
    attend_any(((0, HALF, 0, ROWS), (HALF, HALF, 0, ROWS)), pads, peak_ref, k_ref, v_ref, q_ref, m_ref)
    finished(places)


def aligned_attention(meta, peak, keys, values, queries, cells):
    return pl.pallas_call(
        aligned_kernel,
        out_shape=(shape((C, ROWS)), shape((CELLS, CELL, C)), shape((CELLS, CELL), I32)),
        in_specs=[hbm()] * 6,
        out_specs=(vmem(), hbm(), vmem()),
        scratch_shapes=[
            pltpu.SMEM((CELLS, CELL), I32),
            pltpu.SMEM((CELLS, CELL), F32),
            pltpu.VMEM((ROWS, C), BF16),
            pltpu.VMEM((C, ROWS), BF16),
            pltpu.VMEM((C, ROWS), BF16),
            dma(4), dma(2, CELLS),
        ],
        compiler_params=pltpu.CompilerParams(vmem_limit_bytes=48 * 2**20),
        name="aligned_attention",
    )(meta, peak, keys, values, queries, cells)


def along(step):
    n_grp, n_seq = lax.axis_size("grp"), lax.axis_size("seq")
    flat = lax.axis_index("grp") * n_seq + lax.axis_index("seq")
    other = lax.rem(flat + step + n_grp * n_seq, n_grp * n_seq)
    return (other // n_seq, lax.rem(other, n_seq))


def middle_kernel(
    note_ref, x_hbm, m_hbm, norm_ref, qkv_hbm, out_hbm, up_hbm, down_hbm,
    y_hbm, k_hbm, v_hbm, q_hbm, all_count_ref, peak_ref,
    x_ref, m_ref, qkv_ref, out_ref, up_ref, down_ref,
    y_ref, before_ref, after_ref, note_before, note_after, w_ref, k_ref, v_ref, q_ref,
    load_sem, store_sem, send_before, send_after, recv_before, recv_after, note_send, note_recv,
):
    after, before = along(1), along(-1)
    barrier = pltpu.get_barrier_semaphore()
    for device in (after, before):
        pl.semaphore_signal(barrier, inc=1, device_id=device, device_id_type=MESH)
    loads = started(
        (x_hbm, x_ref, load_sem.at[0]),
        (m_hbm, m_ref, load_sem.at[1]),
        (out_hbm.at[0], out_ref, load_sem.at[2]),
        (up_hbm.at[0], up_ref, load_sem.at[3]),
        (down_hbm.at[0], down_ref, load_sem.at[4]),
        (qkv_hbm.at[1], qkv_ref, load_sem.at[5]),
    )
    finished(loads[5:])
    turn(qkv_ref, w_ref)
    finished(loads[:5])
    pl.semaphore_wait(barrier, 2)
    notes = [
        pltpu.make_async_remote_copy(
            note_ref, target, note_send.at[i], note_recv.at[i], device_id=device, device_id_type=MESH)
        for i, (target, device) in enumerate(((note_after, before), (note_before, after)))
    ]
    for copy in notes:
        copy.start()
    gain, offset = norm_ref[1, 0:1, :], norm_ref[1, 1:2, :]
    peak_ref[...] = jnp.zeros_like(peak_ref)

    def to_before(i):
        return pltpu.make_async_remote_copy(
            y_ref.at[pl.ds(i * STEP, STEP)], after_ref.at[pl.ds(i * STEP, STEP)],
            send_before.at[i], recv_after.at[i], device_id=before, device_id_type=MESH)

    def to_after(i):
        return pltpu.make_async_remote_copy(
            y_ref.at[pl.ds(HALF + i * STEP, STEP)], before_ref.at[pl.ds(i * STEP, STEP)],
            send_after.at[i], recv_before.at[i], device_id=after, device_id_type=MESH)

    def place(rows, pair, k_at, q_at):
        wide = rows.astype(F32)
        wide = jnp.concatenate(
            [first_valid(wide[u * CELL : (u + 1) * CELL], pair[u]) for u in range(2)], axis=0)
        valid = jnp.concatenate([lane_valid(pair[u]) for u in range(2)], axis=1)
        project(
            wide, valid, gain, offset, w_ref[...], qkv_ref[:, C : 2 * C],
            k_ref, v_ref, q_ref, peak_ref, k_at, q_at,
        )

    for i in range(2):
        for chunk, copy in ((i, to_before(i)), (2 + i, to_after(i))):
            at = chunk * STEP
            cells = (2 * chunk, 2 * chunk + 1)
            rows = jnp.concatenate([x_ref[p] for p in cells], axis=0)
            mixture = m_ref[:, at : at + STEP]
            done = finish(
                rows, mixture, norm_ref[0, 2:3, :], norm_ref[0, 3:4, :],
                out_ref[...], up_ref[...], down_ref[...],
            )
            y_ref[at : at + STEP, :] = done
            place(done, [note_ref[p : p + 1, 0:1] for p in cells], HALF + at, at)
            copy.start()
    own = pl.ds(HALF, ROWS)
    stores = started(
        (y_ref, y_hbm, store_sem.at[0]),
        (k_ref.at[own, :], k_hbm.at[own, :], store_sem.at[1]),
        (v_ref.at[:, own], v_hbm.at[:, own], store_sem.at[2]),
        (q_ref, q_hbm, store_sem.at[3]),
    )
    for copy in notes:
        copy.wait()
    for i in range(2):
        for incoming, source, note, first, k_first, at_sem in (
            (to_before(i), after_ref, note_after, 2 * i, HALF + ROWS, 4),
            (to_after(i), before_ref, note_before, CELLS // 2 + 2 * i, 0, 8),
        ):
            incoming.wait_recv()
            pair = [note[first + u : first + u + 1, 0:1] for u in range(2)]
            k_at = k_first + i * STEP
            place(source[i * STEP : (i + 1) * STEP, :], pair, k_at, None)
            part = pl.ds(k_at, STEP)
            stores += started(
                (k_ref.at[part, :], k_hbm.at[part, :], store_sem.at[at_sem + 2 * i]),
                (v_ref.at[:, part], v_hbm.at[:, part], store_sem.at[at_sem + 2 * i + 1]),
            )
    all_count_ref[0:4, :] = note_before[4:8, :]
    all_count_ref[4:12, :] = note_ref[...]
    all_count_ref[12:16, :] = note_after[0:4, :]
    widest(peak_ref)
    for i in range(2):
        to_before(i).wait_send()
        to_after(i).wait_send()
    finished(stores)


def middle(notes, cells, mixture, norms, qkv, out_w, up_w, down_w):
    return pl.pallas_call(
        middle_kernel,
        out_shape=(
            shape((ROWS, C)), shape((2 * ROWS, C)), shape((C, 2 * ROWS)), shape((C, ROWS)),
            shape((2 * CELLS, CELL), I32), shape((CELLS, CELL), F32),
        ),
        in_specs=[vmem()] + [hbm()] * 2 + [vmem()] + [hbm()] * 4,
        out_specs=(hbm(),) * 4 + (vmem(), vmem()),
        scratch_shapes=[
            pltpu.VMEM((CELLS, CELL, C), BF16),
            pltpu.VMEM((C, ROWS), BF16),
            pltpu.VMEM((C, 3 * C), BF16),
            pltpu.VMEM((C, C), BF16),
            pltpu.VMEM((C, HID), BF16),
            pltpu.VMEM((HID, C), BF16),
            pltpu.VMEM((ROWS, C), BF16),
            pltpu.VMEM((HALF, C), BF16),
            pltpu.VMEM((HALF, C), BF16),
            pltpu.VMEM((CELLS, CELL), I32),
            pltpu.VMEM((CELLS, CELL), I32),
            pltpu.VMEM((2 * C, C), BF16),
            pltpu.VMEM((2 * ROWS, C), BF16),
            pltpu.VMEM((C, 2 * ROWS), BF16),
            pltpu.VMEM((C, ROWS), BF16),
            dma(6), dma(12), dma(2), dma(2), dma(2), dma(2), dma(2), dma(2),
        ],
        compiler_params=pltpu.CompilerParams(
            collective_id=1, has_side_effects=True, vmem_limit_bytes=40 * 2**20),
        name="middle",
    )(notes, cells, mixture, norms, qkv, out_w, up_w, down_w)


def shifted_kernel(
    count_hbm, peak_hbm, k_hbm, v_hbm, q_hbm, x_hbm, norm_ref, out_hbm, up_hbm, down_hbm,
    y_hbm,
    count_ref, peak_ref, k_ref, v_ref, q_ref, x_ref, out_ref, up_ref, down_ref, m_ref, y_ref,
    load_sem, store_sem,
):
    loads = started(
        (k_hbm, k_ref, load_sem.at[0]), (q_hbm, q_ref, load_sem.at[1]), (v_hbm, v_ref, load_sem.at[2]),
        (count_hbm, count_ref, load_sem.at[3]), (peak_hbm, peak_ref, load_sem.at[4]),
        (x_hbm, x_ref, load_sem.at[5]), (out_hbm.at[1], out_ref, load_sem.at[6]),
        (up_hbm.at[1], up_ref, load_sem.at[7]), (down_hbm.at[1], down_ref, load_sem.at[8]),
    )
    finished(loads[:5])
    pads = [(CELL - count_ref[j, 0]).astype(F32) for j in range(2 * CELLS)]
    attend_any(((0, HALF, 0, ROWS), (HALF, HALF, ROWS, ROWS)), pads, peak_ref, k_ref, v_ref, q_ref, m_ref)
    finished(loads[5:])
    stores = []
    for i in range(ROWS // STEP):
        at = i * STEP
        done = finish(
            x_ref[at : at + STEP, :], m_ref[:, at : at + STEP], norm_ref[1, 2:3, :], norm_ref[1, 3:4, :],
            out_ref[...], up_ref[...], down_ref[...],
        )
        for u in range(2):
            index = lax.broadcasted_iota(I32, (CELL, 1), 0)
            keep = index < count_ref[CELLS // 2 + 2 * i + u, 0]
            part = done[u * CELL : (u + 1) * CELL, :]
            y_ref[at + u * CELL : at + (u + 1) * CELL, :] = jnp.where(keep, part, jnp.zeros_like(part))
        rows = pl.ds(at, STEP)
        stores += started((y_ref.at[rows], y_hbm.at[rows], store_sem.at[i]))
    finished(stores)


def shifted_block(counts, peak, keys, values, queries, rows, norms, out_w, up_w, down_w):
    return pl.pallas_call(
        shifted_kernel,
        out_shape=shape((ROWS, C)),
        in_specs=[hbm()] * 6 + [vmem()] + [hbm()] * 3,
        out_specs=hbm(),
        scratch_shapes=[
            pltpu.SMEM((2 * CELLS, CELL), I32),
            pltpu.SMEM((CELLS, CELL), F32),
            pltpu.VMEM((2 * ROWS, C), BF16),
            pltpu.VMEM((C, 2 * ROWS), BF16),
            pltpu.VMEM((C, ROWS), BF16),
            pltpu.VMEM((ROWS, C), BF16),
            pltpu.VMEM((C, C), BF16),
            pltpu.VMEM((C, HID), BF16),
            pltpu.VMEM((HID, C), BF16),
            pltpu.VMEM((C, ROWS), BF16),
            pltpu.VMEM((ROWS, C), BF16),
            dma(9), dma(4),
        ],
        compiler_params=pltpu.CompilerParams(vmem_limit_bytes=48 * 2**20),
        name="shifted_block",
    )(counts, peak, keys, values, queries, rows, norms, out_w, up_w, down_w)


def body(points, hilbert_pos, valid_counts, norms, qkv, out_w, up_w, down_w):
    cells, keys, values, queries, meta, peak = gather_cells(
        hilbert_pos, valid_counts, points.reshape(CELLS, CELL, C), norms, qkv)
    mixture, placed, notes = aligned_attention(meta, peak, keys, values, queries, cells)
    rows, keys, values, queries, counts, peak = middle(notes, placed, mixture, norms, qkv, out_w, up_w, down_w)
    return shifted_block(counts, peak, keys, values, queries, rows, norms, out_w, up_w, down_w)


def solution(mesh):
    return jax.shard_map(
        body,
        mesh=mesh,
        in_specs=(
            P(("grp", "seq"), None), P(("grp", "seq")), P(("grp", "seq")), P(), P(), P(), P(), P(),
        ),
        out_specs=P(("grp", "seq"), None),
        check_vma=False,
    )
```

```python
import math

import jax
import jax.numpy as jnp
from jax import lax
from jax.experimental import pallas as pl
from jax.experimental.pallas import tpu as pltpu
from jax.sharding import PartitionSpec as P

C = 256
HEADS = 16
HD = 16
HID = 1024
CELL = 128
CELLS = 8
ROWS = CELL * CELLS
HALF = ROWS // 2
STEP = 2 * CELL
F32 = jnp.float32
BF16 = jnp.bfloat16
I32 = jnp.int32
MESH = pl.DeviceIdType.MESH
SCORE_SCALE = HD**-0.5 * math.log2(math.e)
SAFE_EXPONENT = 60.0
SAFE_VALUE = 2.0**40


def nt_dot(a, b):
    return lax.dot_general(a, b, (((1,), (1,)), ((), ())), preferred_element_type=F32)


def nn_dot(a, b):
    return jnp.dot(a, b, preferred_element_type=F32)


def norm_rows_of(values, gain, offset):
    center = jnp.mean(values, axis=-1, keepdims=True)
    spread = values - center
    second = jnp.mean(spread * spread, axis=-1, keepdims=True)
    return spread * lax.rsqrt(second + 1e-5) * gain + offset


def head_pick(rows, columns, channel_axis):
    channel = lax.broadcasted_iota(I32, (rows, columns), channel_axis) // HD
    head = lax.broadcasted_iota(I32, (rows, columns), 1 - channel_axis)
    return jnp.where(channel == head, 1.0, 0.0).astype(BF16)


def first_valid(rows, count):
    index = lax.broadcasted_iota(I32, (CELL, 1), 0)
    return jnp.where(index < count, rows, rows[0:1, :])


def lane_valid(count):
    return jnp.where(lax.broadcasted_iota(I32, (1, CELL), 1) < count, 1.0, 0.0)


def project(rows, valid, gain, offset, w_t, w_k, k_ref, v_ref, q_ref, peak_ref, k_at, q_at):
    count = rows.shape[0]
    normed = norm_rows_of(rows, gain, offset).astype(BF16)
    keys = nn_dot(normed, w_k).astype(BF16)
    k_ref[pl.ds(k_at, count), :] = keys
    values = nt_dot(w_t[C:, :], normed) * valid
    v_ref[:, pl.ds(k_at, count)] = values.astype(BF16)
    wide = keys.astype(F32)
    sums = nn_dot((wide * wide).astype(BF16), head_pick(C, CELL, 0))
    peak_ref[0:1, :] = jnp.maximum(peak_ref[0:1, :], jnp.max(sums, axis=0, keepdims=True))
    tall = jnp.max(jnp.abs(values), axis=0, keepdims=True)
    peak_ref[2:3, :] = jnp.maximum(peak_ref[2:3, :], jnp.maximum(tall[:, :CELL], tall[:, count - CELL :]))
    if q_at is not None:
        queries = nt_dot(w_t[:C, :], normed).astype(BF16)
        q_ref[:, pl.ds(q_at, count)] = queries
        wide = queries.astype(F32)
        sums = nn_dot(head_pick(HEADS, C, 1), (wide * wide).astype(BF16))
        tall = jnp.max(sums, axis=0, keepdims=True)
        peak_ref[1:2, :] = jnp.maximum(peak_ref[1:2, :], jnp.maximum(tall[:, :CELL], tall[:, count - CELL :]))


def turn(qkv_ref, w_ref):
    for at, source in ((0, 0), (C, 2 * C)):
        w_ref[at : at + C, :] = qkv_ref[:, source : source + C].astype(F32).T.astype(BF16)


def attend(windows, pads, k_ref, v_ref, q_ref, m_ref, exact, unroll):
    def one_head(head):
        row = pl.multiple_of(head * HD, HD)
        half = pl.ds(pl.multiple_of((head // 8) * CELL, CELL), CELL)
        for q_lo, q_n, k_lo, k_n in windows:
            lane_head = lax.broadcasted_iota(I32, (CELL, q_n), 0) // HD
            queries = q_ref[half, q_lo : q_lo + q_n]
            queries = jnp.where(lane_head == head % 8, queries, jnp.zeros_like(queries))
            scores = nn_dot(k_ref[k_lo : k_lo + k_n, half], queries)
            if exact:
                scores = scores - jnp.max(scores, axis=0, keepdims=True)
            weights = jnp.exp2(scores * SCORE_SCALE)
            total = jnp.sum(jnp.sum(weights.reshape(k_n // 8, 8, q_n), axis=0), axis=0, keepdims=True)
            for cell in range(k_n // CELL):
                total = total - pads[k_lo // CELL + cell] * weights[cell * CELL : cell * CELL + 1, :]
            mixed = nn_dot(v_ref[pl.ds(row, HD), k_lo : k_lo + k_n], weights.astype(BF16))
            m_ref[pl.ds(row, HD), q_lo : q_lo + q_n] = (mixed / total).astype(BF16)

    def step(i, carry):
        for u in range(unroll):
            one_head(i * unroll + u)
        return carry

    lax.fori_loop(0, HEADS // unroll, step, 0)


def attend_any(windows, pads, peak_ref, k_ref, v_ref, q_ref, m_ref):
    bound = peak_ref[0:1, :] * peak_ref[1:2, :] * SCORE_SCALE**2
    off = (bound >= SAFE_EXPONENT * SAFE_EXPONENT) | (peak_ref[2:3, :] >= SAFE_VALUE)
    safe = jnp.max(jnp.where(off, 1.0, 0.0)) < 0.5

    @pl.when(safe)
    def _():
        attend(windows, pads, k_ref, v_ref, q_ref, m_ref, False, 4)

    @pl.when(jnp.logical_not(safe))
    def _():
        attend(windows, pads, k_ref, v_ref, q_ref, m_ref, True, 1)


def gelu(values):
    return 0.5 * values * (1.0 + lax.erf(values * (2.0**-0.5)))


def finish(rows, mixture_t, gain, offset, out_w, up_w, down_w):
    residual = rows.astype(F32) + nn_dot(mixture_t.astype(F32).T.astype(BF16), out_w)
    residual = residual.astype(BF16).astype(F32)
    normed = norm_rows_of(residual, gain, offset).astype(BF16)
    hidden = gelu(nn_dot(normed, up_w)).astype(BF16)
    return (residual + nn_dot(hidden, down_w)).astype(BF16)


def widest(peak_ref):
    peak_ref[...] = jnp.broadcast_to(jnp.max(peak_ref[...], axis=1, keepdims=True), peak_ref.shape)


def started(*pairs):
    copies = [pltpu.make_async_copy(*pair) for pair in pairs]
    for copy in copies:
        copy.start()
    return copies


def finished(copies):
    for copy in copies:
        copy.wait()


def gather_kernel(
    pos_hbm, count_hbm, x_hbm, norm_hbm, qkv_hbm,
    cells_ref, k_ref, v_ref, q_ref, meta_ref, peak_ref,
    pos_ref, count_ref, x_buf, norm_ref, out_buf, note_out, note_in, qkv_ref, w_ref,
    load_sem, x_sem, send, recv, note_send, note_recv,
):
    me, seq = lax.axis_index("grp"), lax.axis_index("seq")
    x_loads = started(*((x_hbm.at[j], x_buf.at[j], x_sem.at[j]) for j in range(CELLS)))
    loads = started(
        (pos_hbm, pos_ref, load_sem.at[0]), (count_hbm, count_ref, load_sem.at[1]),
        (norm_hbm, norm_ref, load_sem.at[2]), (qkv_hbm.at[0], qkv_ref, load_sem.at[3]),
    )

    def partner(i, sign):
        hop = i // 2
        hop = jnp.where(hop == 2, 3, jnp.where(hop == 3, 2, hop))
        chip = lax.rem(me // 2 + sign * hop + CELLS // 2, CELLS // 2)
        return chip * 2 + lax.rem(me + i, 2)

    barrier = pltpu.get_barrier_semaphore()
    for i in range(1, CELLS):
        pl.semaphore_signal(barrier, inc=1, device_id=(partner(i, 1), seq), device_id_type=MESH)
    finished(loads[:2])
    finished(x_loads)
    row = lax.broadcasted_iota(I32, (CELLS, CELL), 0)
    for owner in range(CELLS):
        index, place, count = jnp.int32(0), jnp.int32(0), jnp.int32(0)
        for j in range(CELLS):
            position = pos_ref[j]
            mine = position // CELLS == owner
            index = jnp.where(mine, j, index)
            place = jnp.where(mine, position % CELLS, place)
            count = jnp.where(mine, count_ref[j], count)
        out_buf[owner] = x_buf[index]
        note_out[owner] = jnp.where(row == 0, place, count)
    pl.semaphore_wait(barrier, CELLS - 1)

    def sent(i):
        owner = partner(i, 1)
        return (
            pltpu.make_async_remote_copy(
                out_buf.at[owner], cells_ref.at[me], send.at[i], recv.at[i],
                device_id=(owner, seq), device_id_type=MESH),
            pltpu.make_async_remote_copy(
                note_out.at[owner], note_in.at[me], note_send.at[i], note_recv.at[i],
                device_id=(owner, seq), device_id_type=MESH),
        )

    copies = [sent(i) for i in range(CELLS - 1, 0, -1)]
    for pair in copies:
        for copy in pair:
            copy.start()
    finished(loads[2:])
    turn(qkv_ref, w_ref)
    gain, offset = norm_ref[0, 0:1, :], norm_ref[0, 1:2, :]
    peak_ref[...] = jnp.zeros_like(peak_ref)

    def take(j):
        at = pl.multiple_of(j * CELL, CELL)
        count = note_in[j, 1:2, :]
        rows = first_valid(cells_ref[j].astype(F32), count[:, 0:1])
        project(
            rows, lane_valid(count), gain, offset, w_ref[...], qkv_ref[:, C : 2 * C],
            k_ref, v_ref, q_ref, peak_ref, at, at,
        )

    cells_ref[me] = out_buf[me]
    note_in[me] = note_out[me]
    take(me)

    def arrive(i, carry):
        for copy in sent(i):
            copy.wait_recv()
        take(partner(i, -1))
        return carry

    lax.fori_loop(1, CELLS, arrive, 0)
    lane = lax.broadcasted_iota(I32, (CELLS, CELL), 1)
    meta = jnp.zeros((CELLS, CELL), I32)
    for j in range(CELLS):
        meta = jnp.where(lane == j, note_in[j], meta)
    meta_ref[...] = meta
    widest(peak_ref)
    for pair in copies:
        for copy in pair:
            copy.wait_send()


def vmem():
    return pl.BlockSpec(memory_space=pltpu.VMEM)


def hbm():
    return pl.BlockSpec(memory_space=pltpu.HBM)


def shape(dims, dtype=BF16):
    return jax.ShapeDtypeStruct(dims, dtype)


def dma(*dims):
    return pltpu.SemaphoreType.DMA(dims)


def gather_cells(pos, counts, cells, norms, qkv):
    return pl.pallas_call(
        gather_kernel,
        out_shape=(
            shape((CELLS, CELL, C)), shape((ROWS, C)), shape((C, ROWS)), shape((C, ROWS)),
            shape((CELLS, CELL), I32), shape((CELLS, CELL), F32),
        ),
        in_specs=[hbm()] * 5,
        out_specs=(vmem(),) * 6,
        scratch_shapes=[
            pltpu.SMEM((CELLS,), I32),
            pltpu.SMEM((CELLS,), I32),
            pltpu.VMEM((CELLS, CELL, C), BF16),
            pltpu.VMEM((2, 4, C), F32),
            pltpu.VMEM((CELLS, CELL, C), BF16),
            pltpu.VMEM((CELLS, CELLS, CELL), I32),
            pltpu.VMEM((CELLS, CELLS, CELL), I32),
            pltpu.VMEM((C, 3 * C), BF16),
            pltpu.VMEM((2 * C, C), BF16),
            dma(4), dma(CELLS), dma(CELLS), dma(CELLS), dma(CELLS), dma(CELLS),
        ],
        compiler_params=pltpu.CompilerParams(
            collective_id=0, has_side_effects=True, vmem_limit_bytes=24 * 2**20),
        name="gather_cells",
    )(pos, counts, cells, norms, qkv)


def aligned_kernel(
    meta_ref, peak_ref, k_ref, v_ref, q_ref, cells_ref, m_ref, placed_ref, count_ref,
    place_ref, mix_ref, sem,
):
    loads = started((meta_ref, place_ref, sem.at[0]))
    pads = [(CELL - meta_ref[1:2, j : j + 1]).astype(F32) for j in range(CELLS)]
    attend_any(((0, HALF, 0, ROWS), (HALF, HALF, 0, ROWS)), pads, peak_ref, k_ref, v_ref, q_ref, mix_ref)
    finished(loads)
    for j in range(CELLS):
        to = place_ref[0, j]
        m_ref[:, pl.ds(pl.multiple_of(to * CELL, CELL), CELL)] = mix_ref[:, j * CELL : (j + 1) * CELL]
        placed_ref[to] = cells_ref[j]
        count_ref[pl.ds(to, 1), :] = jnp.full((1, CELL), place_ref[1, j], I32)


def aligned_attention(meta, peak, keys, values, queries, cells):
    return pl.pallas_call(
        aligned_kernel,
        out_shape=(shape((C, ROWS)), shape((CELLS, CELL, C)), shape((CELLS, CELL), I32)),
        in_specs=[vmem()] * 6,
        out_specs=(vmem(),) * 3,
        scratch_shapes=[
            pltpu.SMEM((CELLS, CELL), I32),
            pltpu.VMEM((C, ROWS), BF16),
            dma(1),
        ],
        compiler_params=pltpu.CompilerParams(vmem_limit_bytes=40 * 2**20),
        name="aligned_attention",
    )(meta, peak, keys, values, queries, cells)


def along(step):
    n_grp, n_seq = lax.axis_size("grp"), lax.axis_size("seq")
    flat = lax.axis_index("grp") * n_seq + lax.axis_index("seq")
    other = lax.rem(flat + step + n_grp * n_seq, n_grp * n_seq)
    return (other // n_seq, lax.rem(other, n_seq))


def middle_kernel(
    note_ref, x_ref, m_ref, norm_ref, qkv_ref, out_ref, up_ref, down_ref,
    y_ref, k_ref, v_ref, q_ref, all_count_ref, peak_ref,
    before_ref, after_ref, note_before, note_after, w_ref,
    send_before, send_after, recv_before, recv_after, note_send, note_recv,
):
    after, before = along(1), along(-1)
    barrier = pltpu.get_barrier_semaphore()
    for device in (after, before):
        pl.semaphore_signal(barrier, inc=1, device_id=device, device_id_type=MESH)
    turn(qkv_ref.at[1], w_ref)
    gain, offset = norm_ref[1, 0:1, :], norm_ref[1, 1:2, :]
    peak_ref[...] = jnp.zeros_like(peak_ref)
    notes = [
        pltpu.make_async_remote_copy(
            note_ref, target, note_send.at[i], note_recv.at[i], device_id=device, device_id_type=MESH)
        for i, (target, device) in enumerate(((note_after, before), (note_before, after)))
    ]

    def to_before(i):
        return pltpu.make_async_remote_copy(
            y_ref.at[pl.ds(i * STEP, STEP)], after_ref.at[pl.ds(i * STEP, STEP)],
            send_before.at[i], recv_after.at[i], device_id=before, device_id_type=MESH)

    def to_after(i):
        return pltpu.make_async_remote_copy(
            y_ref.at[pl.ds(HALF + i * STEP, STEP)], before_ref.at[pl.ds(i * STEP, STEP)],
            send_after.at[i], recv_before.at[i], device_id=after, device_id_type=MESH)

    def place(rows, pair, k_at, q_at):
        wide = rows.astype(F32)
        wide = jnp.concatenate(
            [first_valid(wide[u * CELL : (u + 1) * CELL], pair[u]) for u in range(2)], axis=0)
        valid = jnp.concatenate([lane_valid(pair[u]) for u in range(2)], axis=1)
        project(
            wide, valid, gain, offset, w_ref[...], qkv_ref[1, :, C : 2 * C],
            k_ref, v_ref, q_ref, peak_ref, k_at, q_at,
        )

    for i in range(2):
        for chunk, copy in ((i, to_before(i)), (2 + i, to_after(i))):
            at = chunk * STEP
            cells = (2 * chunk, 2 * chunk + 1)
            done = finish(
                jnp.concatenate([x_ref[p] for p in cells], axis=0), m_ref[:, at : at + STEP],
                norm_ref[0, 2:3, :], norm_ref[0, 3:4, :], out_ref[0], up_ref[0], down_ref[0],
            )
            y_ref[at : at + STEP, :] = done
            place(done, [note_ref[p : p + 1, 0:1] for p in cells], HALF + at, at)
            if i == 0 and chunk == 0:
                pl.semaphore_wait(barrier, 2)
                for note in notes:
                    note.start()
            copy.start()
    for copy in notes:
        copy.wait()
    for i in range(2):
        for incoming, source, note, first, k_first in (
            (to_before(i), after_ref, note_after, 2 * i, HALF + ROWS),
            (to_after(i), before_ref, note_before, CELLS // 2 + 2 * i, 0),
        ):
            incoming.wait_recv()
            pair = [note[first + u : first + u + 1, 0:1] for u in range(2)]
            place(source[i * STEP : (i + 1) * STEP, :], pair, k_first + i * STEP, None)
    all_count_ref[0:4, :] = note_before[4:8, :]
    all_count_ref[4:12, :] = note_ref[...]
    all_count_ref[12:16, :] = note_after[0:4, :]
    widest(peak_ref)
    for i in range(2):
        to_before(i).wait_send()
        to_after(i).wait_send()


def middle(notes, cells, mixture, norms, qkv, out_w, up_w, down_w):
    return pl.pallas_call(
        middle_kernel,
        out_shape=(
            shape((ROWS, C)), shape((2 * ROWS, C)), shape((C, 2 * ROWS)), shape((C, ROWS)),
            shape((2 * CELLS, CELL), I32), shape((CELLS, CELL), F32),
        ),
        in_specs=[vmem()] * 8,
        out_specs=(vmem(),) * 6,
        scratch_shapes=[
            pltpu.VMEM((HALF, C), BF16),
            pltpu.VMEM((HALF, C), BF16),
            pltpu.VMEM((CELLS, CELL), I32),
            pltpu.VMEM((CELLS, CELL), I32),
            pltpu.VMEM((2 * C, C), BF16),
            dma(2), dma(2), dma(2), dma(2), dma(2), dma(2),
        ],
        compiler_params=pltpu.CompilerParams(
            collective_id=1, has_side_effects=True, vmem_limit_bytes=32 * 2**20),
        name="middle",
    )(notes, cells, mixture, norms, qkv, out_w, up_w, down_w)


def shifted_kernel(
    count_ref, peak_ref, k_ref, v_ref, q_ref, x_ref, norm_ref, out_ref, up_ref, down_ref,
    y_hbm, m_ref, y_ref, store_sem,
):
    pads = [(CELL - count_ref[j : j + 1, 0:1]).astype(F32) for j in range(2 * CELLS)]
    attend_any(((0, HALF, 0, ROWS), (HALF, HALF, ROWS, ROWS)), pads, peak_ref, k_ref, v_ref, q_ref, m_ref)
    stores = []
    for i in range(ROWS // STEP):
        at = i * STEP
        done = finish(
            x_ref[at : at + STEP, :], m_ref[:, at : at + STEP], norm_ref[1, 2:3, :], norm_ref[1, 3:4, :],
            out_ref[1], up_ref[1], down_ref[1],
        )
        for u in range(2):
            cell = CELLS // 2 + 2 * i + u
            keep = lax.broadcasted_iota(I32, (CELL, 1), 0) < count_ref[cell : cell + 1, 0:1]
            part = done[u * CELL : (u + 1) * CELL, :]
            y_ref[at + u * CELL : at + (u + 1) * CELL, :] = jnp.where(keep, part, jnp.zeros_like(part))
        rows = pl.ds(at, STEP)
        stores += started((y_ref.at[rows], y_hbm.at[rows], store_sem.at[i]))
    finished(stores)


def shifted_block(counts, peak, keys, values, queries, rows, norms, out_w, up_w, down_w):
    return pl.pallas_call(
        shifted_kernel,
        out_shape=shape((ROWS, C)),
        in_specs=[vmem()] * 10,
        out_specs=hbm(),
        scratch_shapes=[
            pltpu.VMEM((C, ROWS), BF16),
            pltpu.VMEM((ROWS, C), BF16),
            dma(4),
        ],
        compiler_params=pltpu.CompilerParams(vmem_limit_bytes=40 * 2**20),
        name="shifted_block",
    )(counts, peak, keys, values, queries, rows, norms, out_w, up_w, down_w)


def body(points, hilbert_pos, valid_counts, norms, qkv, out_w, up_w, down_w):
    cells, keys, values, queries, meta, peak = gather_cells(*(
        pltpu.with_memory_space_constraint(array, pltpu.HBM)
        for array in (hilbert_pos, valid_counts, points.reshape(CELLS, CELL, C), norms, qkv)))
    mixture, placed, notes = aligned_attention(meta, peak, keys, values, queries, cells)
    rows, keys, values, queries, counts, peak = middle(notes, placed, mixture, norms, qkv, out_w, up_w, down_w)
    return shifted_block(counts, peak, keys, values, queries, rows, norms, out_w, up_w, down_w)


def solution(mesh):
    return jax.shard_map(
        body,
        mesh=mesh,
        in_specs=(
            P(("grp", "seq"), None), P(("grp", "seq")), P(("grp", "seq")), P(), P(), P(), P(), P(),
        ),
        out_specs=P(("grp", "seq"), None),
        check_vma=False,
    )
```

```python
import math

import jax
import jax.numpy as jnp
from jax import lax
from jax.experimental import pallas as pl
from jax.experimental.pallas import tpu as pltpu
from jax.sharding import PartitionSpec as P

C = 256
HEADS = 16
HD = 16
HID = 1024
CELL = 128
CELLS = 8
ROWS = CELL * CELLS
HALF = ROWS // 2
STEP = 2 * CELL
F32 = jnp.float32
BF16 = jnp.bfloat16
I32 = jnp.int32
MESH = pl.DeviceIdType.MESH
SCORE_SCALE = HD**-0.5 * math.log2(math.e)
SAFE_EXPONENT = 60.0
SAFE_VALUE = 2.0**40
UNROLL = 4
EARLY = ((0, HALF, 0, HALF, False, False),)
LATE = ((0, HALF, HALF, HALF, True, True), (HALF, HALF, 0, ROWS, False, True))
ALIGNED = ((0, HALF, 0, ROWS, False, True), (HALF, HALF, 0, ROWS, False, True))
OWN = ((0, HALF, HALF, HALF, False, False), (HALF, HALF, ROWS, HALF, False, False))
BORROWED = ((0, HALF, 0, HALF, True, True), (HALF, HALF, ROWS + HALF, HALF, True, True))
SHIFTED = ((0, HALF, 0, ROWS, False, True), (HALF, HALF, ROWS, ROWS, False, True))


def nt_dot(a, b):
    return lax.dot_general(a, b, (((1,), (1,)), ((), ())), preferred_element_type=F32)


def nn_dot(a, b):
    return jnp.dot(a, b, preferred_element_type=F32)


def norm_rows_of(values, gain, offset):
    center = jnp.mean(values, axis=-1, keepdims=True)
    spread = values - center
    second = jnp.mean(spread * spread, axis=-1, keepdims=True)
    return spread * lax.rsqrt(second + 1e-5) * gain + offset


def head_pick(rows, columns, channel_axis):
    channel = lax.broadcasted_iota(I32, (rows, columns), channel_axis) // HD
    head = lax.broadcasted_iota(I32, (rows, columns), 1 - channel_axis)
    return jnp.where(channel == head, 1.0, 0.0).astype(BF16)


def first_valid(rows, count):
    index = lax.broadcasted_iota(I32, (CELL, 1), 0)
    return jnp.where(index < count, rows, rows[0:1, :])


def lane_valid(count):
    return jnp.where(lax.broadcasted_iota(I32, (1, CELL), 1) < count, 1.0, 0.0)


def project(rows, valid, gain, offset, w_t, w_k, k_ref, v_ref, q_ref, peak_ref, k_at, q_at):
    count = rows.shape[0]
    normed = norm_rows_of(rows, gain, offset).astype(BF16)
    keys = nn_dot(normed, w_k).astype(BF16)
    k_ref[pl.ds(k_at, count), :] = keys
    values = nt_dot(w_t[C:, :], normed) * valid
    v_ref[:, pl.ds(k_at, count)] = values.astype(BF16)
    wide = keys.astype(F32)
    sums = nn_dot((wide * wide).astype(BF16), head_pick(C, CELL, 0))
    peak_ref[0:1, :] = jnp.maximum(peak_ref[0:1, :], jnp.max(sums, axis=0, keepdims=True))
    tall = jnp.max(jnp.abs(values), axis=0, keepdims=True)
    peak_ref[2:3, :] = jnp.maximum(peak_ref[2:3, :], jnp.maximum(tall[:, :CELL], tall[:, count - CELL :]))
    if q_at is not None:
        queries = nt_dot(w_t[:C, :], normed).astype(BF16)
        q_ref[:, pl.ds(q_at, count)] = queries
        wide = queries.astype(F32)
        sums = nn_dot(head_pick(HEADS, C, 1), (wide * wide).astype(BF16))
        tall = jnp.max(sums, axis=0, keepdims=True)
        peak_ref[1:2, :] = jnp.maximum(peak_ref[1:2, :], jnp.maximum(tall[:, :CELL], tall[:, count - CELL :]))


def turn(qkv_ref, w_ref):
    for at, source in ((0, 0), (C, 2 * C)):
        w_ref[at : at + C, :] = qkv_ref[:, source : source + C].astype(F32).T.astype(BF16)


def attend(windows, pads, k_ref, v_ref, q_ref, m_ref, part, exact, unroll):
    def one_head(head):
        row = pl.ds(pl.multiple_of(head * HD, HD), HD)
        half = pl.ds(pl.multiple_of((head // 8) * CELL, CELL), CELL)
        for q_lo, q_n, k_lo, k_n, goes_on, ends in windows:
            q_at = pl.ds(q_lo, q_n)
            lane_head = lax.broadcasted_iota(I32, (CELL, q_n), 0) // HD
            queries = q_ref[half, q_at]
            queries = jnp.where(lane_head == head % 8, queries, jnp.zeros_like(queries))
            scores = nn_dot(k_ref[k_lo : k_lo + k_n, half], queries)
            if exact:
                scores = scores - jnp.max(scores, axis=0, keepdims=True)
            weights = jnp.exp2(scores * SCORE_SCALE)
            total = jnp.sum(jnp.sum(weights.reshape(k_n // 8, 8, q_n), axis=0), axis=0, keepdims=True)
            for cell in range(k_n // CELL):
                total = total - pads[k_lo // CELL + cell] * weights[cell * CELL : cell * CELL + 1, :]
            mixed = nn_dot(v_ref[row, k_lo : k_lo + k_n], weights.astype(BF16))
            if goes_on:
                mixed = mixed + part[0][row, q_at]
                total = total + part[1][pl.ds(head, 1), q_at]
            if ends:
                m_ref[row, q_at] = (mixed / total).astype(BF16)
            else:
                part[0][row, q_at] = mixed
                part[1][pl.ds(head, 1), q_at] = total

    def step(i, carry):
        for u in range(unroll):
            one_head(i * unroll + u)
        return carry

    lax.fori_loop(0, HEADS // unroll, step, 0)


def attend_any(windows, whole_windows, pads, peak_ref, k_ref, v_ref, q_ref, m_ref, part):
    bound = peak_ref[0:1, :] * peak_ref[1:2, :] * SCORE_SCALE**2
    off = (bound >= SAFE_EXPONENT * SAFE_EXPONENT) | (peak_ref[2:3, :] >= SAFE_VALUE)
    safe = jnp.max(jnp.where(off, 1.0, 0.0)) < 0.5

    @pl.when(safe)
    def _():
        attend(windows, pads, k_ref, v_ref, q_ref, m_ref, part, False, UNROLL)

    @pl.when(jnp.logical_not(safe))
    def _():
        attend(whole_windows, pads, k_ref, v_ref, q_ref, m_ref, part, True, 1)


def gelu(values):
    return 0.5 * values * (1.0 + lax.erf(values * (2.0**-0.5)))


def finish(rows, mixture_t, gain, offset, out_w, up_w, down_w):
    residual = rows.astype(F32) + nn_dot(mixture_t.astype(F32).T.astype(BF16), out_w)
    residual = residual.astype(BF16).astype(F32)
    normed = norm_rows_of(residual, gain, offset).astype(BF16)
    hidden = gelu(nn_dot(normed, up_w)).astype(BF16)
    return (residual + nn_dot(hidden, down_w)).astype(BF16)


def widest(peak_ref):
    peak_ref[...] = jnp.broadcast_to(jnp.max(peak_ref[...], axis=1, keepdims=True), peak_ref.shape)


def started(*pairs):
    copies = [pltpu.make_async_copy(*pair) for pair in pairs]
    for copy in copies:
        copy.start()
    return copies


def finished(copies):
    for copy in copies:
        copy.wait()


def gather_kernel(
    pos_hbm, count_hbm, x_hbm, norm_hbm, qkv_hbm,
    cells_ref, k_ref, v_ref, q_ref, meta_ref, peak_ref, mixed_ref, total_ref,
    pos_ref, count_ref, x_buf, norm_ref, out_buf, note_out, note_in, qkv_ref, w_ref,
    load_sem, x_sem, send, recv, note_send, note_recv,
):
    me, seq = lax.axis_index("grp"), lax.axis_index("seq")
    x_loads = started(*((x_hbm.at[j], x_buf.at[j], x_sem.at[j]) for j in range(CELLS)))
    loads = started(
        (pos_hbm, pos_ref, load_sem.at[0]), (count_hbm, count_ref, load_sem.at[1]),
        (norm_hbm, norm_ref, load_sem.at[2]), (qkv_hbm.at[0], qkv_ref, load_sem.at[3]),
    )

    def partner(i):
        hop = i // 2
        hop = 3 if hop == 2 else 2 if hop == 3 else hop
        return lax.rem(me // 2 + hop, CELLS // 2) * 2 + lax.rem(me + i, 2)

    barrier = pltpu.get_barrier_semaphore()
    for i in range(1, CELLS):
        pl.semaphore_signal(barrier, inc=1, device_id=(partner(i), seq), device_id_type=MESH)
    finished(loads[:2])
    finished(x_loads)
    row = lax.broadcasted_iota(I32, (CELLS, CELL), 0)
    for owner in range(CELLS):
        index, place, count = jnp.int32(0), jnp.int32(0), jnp.int32(0)
        for j in range(CELLS):
            position = pos_ref[j]
            mine = position // CELLS == owner
            index = jnp.where(mine, j, index)
            place = jnp.where(mine, position % CELLS, place)
            count = jnp.where(mine, count_ref[j], count)
        out_buf[owner] = x_buf[index]
        note_out[owner] = jnp.where(row == 0, place, count)
    pl.semaphore_wait(barrier, CELLS - 1)

    def sent(i):
        owner = partner(i)
        return (
            pltpu.make_async_remote_copy(
                out_buf.at[owner], cells_ref.at[i], send.at[i], recv.at[i],
                device_id=(owner, seq), device_id_type=MESH),
            pltpu.make_async_remote_copy(
                note_out.at[owner], note_in.at[i], note_send.at[i], note_recv.at[i],
                device_id=(owner, seq), device_id_type=MESH),
        )

    copies = [sent(i) for i in range(1, CELLS)]
    for pair in copies[:5]:
        for copy in pair:
            copy.start()
    finished(loads[2:])
    turn(qkv_ref, w_ref)
    gain, offset = norm_ref[0, 0:1, :], norm_ref[0, 1:2, :]
    peak_ref[...] = jnp.zeros_like(peak_ref)

    def take(j):
        at = pl.multiple_of(j * CELL, CELL)
        count = note_in[j, 1:2, :]
        rows = first_valid(cells_ref[j].astype(F32), count[:, 0:1])
        project(
            rows, lane_valid(count), gain, offset, w_ref[...], qkv_ref[:, C : 2 * C],
            k_ref, v_ref, q_ref, peak_ref, at, at,
        )

    cells_ref[0] = out_buf[me]
    note_in[0] = note_out[me]
    take(0)

    def arrive(i):
        for copy in copies[i - 1]:
            copy.wait_recv()
        take(i)

    arrive(1)
    for pair in copies[:5]:
        for copy in pair:
            copy.wait_send()
    for pair in copies[5:]:
        for copy in pair:
            copy.start()
    arrive(2)
    arrive(3)
    pads = [(CELL - note_in[j, 1:2, 0:1]).astype(F32) for j in range(CELLS // 2)]
    attend(EARLY, pads, k_ref, v_ref, q_ref, None, (mixed_ref, total_ref), False, UNROLL)
    for i in range(4, CELLS):
        arrive(i)
    lane = lax.broadcasted_iota(I32, (CELLS, CELL), 1)
    meta = jnp.zeros((CELLS, CELL), I32)
    for j in range(CELLS):
        meta = jnp.where(lane == j, note_in[j], meta)
    meta_ref[...] = meta
    widest(peak_ref)
    for pair in copies[5:]:
        for copy in pair:
            copy.wait_send()


def vmem():
    return pl.BlockSpec(memory_space=pltpu.VMEM)


def hbm():
    return pl.BlockSpec(memory_space=pltpu.HBM)


def shape(dims, dtype=BF16):
    return jax.ShapeDtypeStruct(dims, dtype)


def dma(*dims):
    return pltpu.SemaphoreType.DMA(dims)


def gather_cells(pos, counts, cells, norms, qkv):
    return pl.pallas_call(
        gather_kernel,
        out_shape=(
            shape((CELLS, CELL, C)), shape((ROWS, C)), shape((C, ROWS)), shape((C, ROWS)),
            shape((CELLS, CELL), I32), shape((CELLS, CELL), F32), shape((C, HALF), F32), shape((HEADS, HALF), F32),
        ),
        in_specs=[hbm()] * 5,
        out_specs=(vmem(),) * 8,
        scratch_shapes=[
            pltpu.SMEM((CELLS,), I32),
            pltpu.SMEM((CELLS,), I32),
            pltpu.VMEM((CELLS, CELL, C), BF16),
            pltpu.VMEM((2, 4, C), F32),
            pltpu.VMEM((CELLS, CELL, C), BF16),
            pltpu.VMEM((CELLS, CELLS, CELL), I32),
            pltpu.VMEM((CELLS, CELLS, CELL), I32),
            pltpu.VMEM((C, 3 * C), BF16),
            pltpu.VMEM((2 * C, C), BF16),
            dma(4), dma(CELLS), dma(CELLS), dma(CELLS), dma(CELLS), dma(CELLS),
        ],
        compiler_params=pltpu.CompilerParams(
            collective_id=0, has_side_effects=True, vmem_limit_bytes=32 * 2**20),
        name="gather_cells",
    )(pos, counts, cells, norms, qkv)


def aligned_kernel(
    meta_ref, peak_ref, k_ref, v_ref, q_ref, cells_ref, mixed_ref, total_ref, m_ref, placed_ref, count_ref,
    place_ref, mix_ref, sem,
):
    loads = started((meta_ref, place_ref, sem.at[0]))
    pads = [(CELL - meta_ref[1:2, j : j + 1]).astype(F32) for j in range(CELLS)]
    attend_any(LATE, ALIGNED, pads, peak_ref, k_ref, v_ref, q_ref, mix_ref, (mixed_ref, total_ref))
    finished(loads)
    for j in range(CELLS):
        to = place_ref[0, j]
        m_ref[:, pl.ds(pl.multiple_of(to * CELL, CELL), CELL)] = mix_ref[:, j * CELL : (j + 1) * CELL]
        placed_ref[to] = cells_ref[j]
        count_ref[pl.ds(to, 1), :] = jnp.full((1, CELL), place_ref[1, j], I32)


def aligned_attention(meta, peak, keys, values, queries, cells, mixed, total):
    return pl.pallas_call(
        aligned_kernel,
        out_shape=(shape((C, ROWS)), shape((CELLS, CELL, C)), shape((CELLS, CELL), I32)),
        in_specs=[vmem()] * 8,
        out_specs=(vmem(),) * 3,
        scratch_shapes=[
            pltpu.SMEM((CELLS, CELL), I32),
            pltpu.VMEM((C, ROWS), BF16),
            dma(1),
        ],
        compiler_params=pltpu.CompilerParams(vmem_limit_bytes=36 * 2**20),
        name="aligned_attention",
    )(meta, peak, keys, values, queries, cells, mixed, total)


def along(step):
    n_grp, n_seq = lax.axis_size("grp"), lax.axis_size("seq")
    flat = lax.axis_index("grp") * n_seq + lax.axis_index("seq")
    other = lax.rem(flat + step + n_grp * n_seq, n_grp * n_seq)
    return (other // n_seq, lax.rem(other, n_seq))


def middle_kernel(
    note_ref, x_ref, m_ref, norm_ref, qkv_ref, out_ref, up_ref, down_ref,
    y_ref, k_ref, v_ref, q_ref, all_count_ref, peak_ref, mixed_ref, total_ref,
    before_ref, after_ref, note_before, note_after, w_ref,
    send_before, send_after, recv_before, recv_after, note_send, note_recv,
):
    after, before = along(1), along(-1)
    barrier = pltpu.get_barrier_semaphore()
    for device in (after, before):
        pl.semaphore_signal(barrier, inc=1, device_id=device, device_id_type=MESH)
    turn(qkv_ref.at[1], w_ref)
    gain, offset = norm_ref[1, 0:1, :], norm_ref[1, 1:2, :]
    peak_ref[...] = jnp.zeros_like(peak_ref)
    notes = [
        pltpu.make_async_remote_copy(
            note_ref, target, note_send.at[i], note_recv.at[i], device_id=device, device_id_type=MESH)
        for i, (target, device) in enumerate(((note_after, before), (note_before, after)))
    ]

    def to_before(i):
        return pltpu.make_async_remote_copy(
            y_ref.at[pl.ds(i * STEP, STEP)], after_ref.at[pl.ds(i * STEP, STEP)],
            send_before.at[i], recv_after.at[i], device_id=before, device_id_type=MESH)

    def to_after(i):
        return pltpu.make_async_remote_copy(
            y_ref.at[pl.ds(HALF + i * STEP, STEP)], before_ref.at[pl.ds(i * STEP, STEP)],
            send_after.at[i], recv_before.at[i], device_id=after, device_id_type=MESH)

    def place(rows, pair, k_at, q_at):
        wide = rows.astype(F32)
        wide = jnp.concatenate(
            [first_valid(wide[u * CELL : (u + 1) * CELL], pair[u]) for u in range(2)], axis=0)
        valid = jnp.concatenate([lane_valid(pair[u]) for u in range(2)], axis=1)
        project(
            wide, valid, gain, offset, w_ref[...], qkv_ref[1, :, C : 2 * C],
            k_ref, v_ref, q_ref, peak_ref, k_at, q_at,
        )

    for i in range(2):
        for chunk, copy in ((i, to_before(i)), (2 + i, to_after(i))):
            at = chunk * STEP
            cells = (2 * chunk, 2 * chunk + 1)
            done = finish(
                jnp.concatenate([x_ref[p] for p in cells], axis=0), m_ref[:, at : at + STEP],
                norm_ref[0, 2:3, :], norm_ref[0, 3:4, :], out_ref[0], up_ref[0], down_ref[0],
            )
            y_ref[at : at + STEP, :] = done
            place(done, [note_ref[p : p + 1, 0:1] for p in cells], HALF + at, at)
            if i == 0 and chunk == 0:
                pl.semaphore_wait(barrier, 2)
                for note in notes:
                    note.start()
            copy.start()
    pads = [None] * 4 + [(CELL - note_ref[p : p + 1, 0:1]).astype(F32) for p in range(CELLS)]
    attend(OWN, pads, k_ref, v_ref, q_ref, None, (mixed_ref, total_ref), False, UNROLL)
    for copy in notes:
        copy.wait()
    for i in range(2):
        for incoming, source, note, first, k_first in (
            (to_before(i), after_ref, note_after, 2 * i, HALF + ROWS),
            (to_after(i), before_ref, note_before, CELLS // 2 + 2 * i, 0),
        ):
            incoming.wait_recv()
            pair = [note[first + u : first + u + 1, 0:1] for u in range(2)]
            place(source[i * STEP : (i + 1) * STEP, :], pair, k_first + i * STEP, None)
    all_count_ref[0:4, :] = note_before[4:8, :]
    all_count_ref[4:12, :] = note_ref[...]
    all_count_ref[12:16, :] = note_after[0:4, :]
    widest(peak_ref)
    for i in range(2):
        to_before(i).wait_send()
        to_after(i).wait_send()


def middle(notes, cells, mixture, norms, qkv, out_w, up_w, down_w):
    return pl.pallas_call(
        middle_kernel,
        out_shape=(
            shape((ROWS, C)), shape((2 * ROWS, C)), shape((C, 2 * ROWS)), shape((C, ROWS)),
            shape((2 * CELLS, CELL), I32), shape((CELLS, CELL), F32), shape((C, ROWS), F32), shape((HEADS, ROWS), F32),
        ),
        in_specs=[vmem()] * 8,
        out_specs=(vmem(),) * 8,
        scratch_shapes=[
            pltpu.VMEM((HALF, C), BF16),
            pltpu.VMEM((HALF, C), BF16),
            pltpu.VMEM((CELLS, CELL), I32),
            pltpu.VMEM((CELLS, CELL), I32),
            pltpu.VMEM((2 * C, C), BF16),
            dma(2), dma(2), dma(2), dma(2), dma(2), dma(2),
        ],
        compiler_params=pltpu.CompilerParams(
            collective_id=1, has_side_effects=True, vmem_limit_bytes=32 * 2**20),
        name="middle",
    )(notes, cells, mixture, norms, qkv, out_w, up_w, down_w)


def shifted_kernel(
    count_ref, peak_ref, k_ref, v_ref, q_ref, mixed_ref, total_ref, x_ref, norm_ref, out_ref, up_ref, down_ref,
    y_hbm, m_ref, y_ref, store_sem,
):
    pads = [(CELL - count_ref[j : j + 1, 0:1]).astype(F32) for j in range(2 * CELLS)]
    attend_any(BORROWED, SHIFTED, pads, peak_ref, k_ref, v_ref, q_ref, m_ref, (mixed_ref, total_ref))
    stores = []
    for i in range(ROWS // STEP):
        at = i * STEP
        done = finish(
            x_ref[at : at + STEP, :], m_ref[:, at : at + STEP], norm_ref[1, 2:3, :], norm_ref[1, 3:4, :],
            out_ref[1], up_ref[1], down_ref[1],
        )
        for u in range(2):
            cell = CELLS // 2 + 2 * i + u
            keep = lax.broadcasted_iota(I32, (CELL, 1), 0) < count_ref[cell : cell + 1, 0:1]
            part = done[u * CELL : (u + 1) * CELL, :]
            y_ref[at + u * CELL : at + (u + 1) * CELL, :] = jnp.where(keep, part, jnp.zeros_like(part))
        rows = pl.ds(at, STEP)
        stores += started((y_ref.at[rows], y_hbm.at[rows], store_sem.at[i]))
    finished(stores)


def shifted_block(counts, peak, keys, values, queries, mixed, total, rows, norms, out_w, up_w, down_w):
    return pl.pallas_call(
        shifted_kernel,
        out_shape=shape((ROWS, C)),
        in_specs=[vmem()] * 12,
        out_specs=hbm(),
        scratch_shapes=[
            pltpu.VMEM((C, ROWS), BF16),
            pltpu.VMEM((ROWS, C), BF16),
            dma(4),
        ],
        compiler_params=pltpu.CompilerParams(vmem_limit_bytes=36 * 2**20),
        name="shifted_block",
    )(counts, peak, keys, values, queries, mixed, total, rows, norms, out_w, up_w, down_w)


def body(points, hilbert_pos, valid_counts, norms, qkv, out_w, up_w, down_w):
    cells, keys, values, queries, meta, peak, mixed, total = gather_cells(*(
        pltpu.with_memory_space_constraint(array, pltpu.HBM)
        for array in (hilbert_pos, valid_counts, points.reshape(CELLS, CELL, C), norms, qkv)))
    mixture, placed, notes = aligned_attention(meta, peak, keys, values, queries, cells, mixed, total)
    rows, keys, values, queries, counts, peak, mixed, total = middle(notes, placed, mixture, norms, qkv, out_w, up_w, down_w)
    return shifted_block(
        counts, peak, keys, values, queries, mixed, total, rows, norms, out_w, up_w, down_w)


def solution(mesh):
    return jax.shard_map(
        body,
        mesh=mesh,
        in_specs=(
            P(("grp", "seq"), None), P(("grp", "seq")), P(("grp", "seq")), P(), P(), P(), P(), P(),
        ),
        out_specs=P(("grp", "seq"), None),
        check_vma=False,
    )
```

```python
import math

import jax
import jax.numpy as jnp
from jax import lax
from jax.experimental import pallas as pl
from jax.experimental.pallas import tpu as pltpu
from jax.sharding import PartitionSpec as P

C = 256
HEADS = 16
HD = 16
HID = 1024
CELL = 128
CELLS = 8
ROWS = CELL * CELLS
HALF = ROWS // 2
STEP = 2 * CELL
F32 = jnp.float32
BF16 = jnp.bfloat16
I32 = jnp.int32
MESH = pl.DeviceIdType.MESH
SCORE_SCALE = HD**-0.5 * math.log2(math.e)
SAFE_EXPONENT = 60.0
SAFE_VALUE = 2.0**40
EARLY = ((0, HALF, 0, HALF, False, False),)
LATER = ((0, HALF, HALF, STEP, True, False),)
LAST = ((0, HALF, HALF + STEP, STEP, True, True),)
OTHERS = ((HALF, HALF, 0, ROWS, False, True),)
ALIGNED = ((0, HALF, 0, ROWS, False, True), (HALF, HALF, 0, ROWS, False, True))
OWN = ((0, HALF, HALF, HALF, False, False), (HALF, HALF, ROWS, HALF, False, False))
BORROWED = ((0, HALF, 0, HALF, True, True), (HALF, HALF, ROWS + HALF, HALF, True, True))
SHIFTED = ((0, HALF, 0, ROWS, False, True), (HALF, HALF, ROWS, ROWS, False, True))


def nt_dot(a, b):
    return lax.dot_general(a, b, (((1,), (1,)), ((), ())), preferred_element_type=F32)


def nn_dot(a, b):
    return jnp.dot(a, b, preferred_element_type=F32)


def norm_rows_of(values, gain, offset):
    center = jnp.mean(values, axis=-1, keepdims=True)
    spread = values - center
    second = jnp.mean(spread * spread, axis=-1, keepdims=True)
    return spread * lax.rsqrt(second + 1e-5) * gain + offset


def head_pick(rows, columns, channel_axis):
    channel = lax.broadcasted_iota(I32, (rows, columns), channel_axis) // HD
    head = lax.broadcasted_iota(I32, (rows, columns), 1 - channel_axis)
    return jnp.where(channel == head, 1.0, 0.0).astype(BF16)


def first_valid(rows, count):
    index = lax.broadcasted_iota(I32, (CELL, 1), 0)
    return jnp.where(index < count, rows, rows[0:1, :])


def lane_valid(count):
    return jnp.where(lax.broadcasted_iota(I32, (1, CELL), 1) < count, 1.0, 0.0)


def raise_peak(peak_ref, row, tall):
    peak = peak_ref[row : row + 1, :]
    for at in range(0, tall.shape[1], CELL):
        peak = jnp.maximum(peak, tall[:, at : at + CELL])
    peak_ref[row : row + 1, :] = peak


def cells_in(rows, counts):
    wide = rows.astype(F32)
    cells = [first_valid(wide[u * CELL : (u + 1) * CELL], count) for u, count in enumerate(counts)]
    return jnp.concatenate(cells, axis=0), jnp.concatenate([lane_valid(count) for count in counts], axis=1)


def project(rows, valid, gain, offset, w_t, w_k, k_ref, v_ref, q_ref, peak_ref, k_at, q_at):
    count = rows.shape[0]
    normed = norm_rows_of(rows, gain, offset).astype(BF16)
    keys = nn_dot(normed, w_k).astype(BF16)
    k_ref[pl.ds(k_at, count), :] = keys
    values = nt_dot(w_t[C:, :], normed) * valid
    v_ref[:, pl.ds(k_at, count)] = values.astype(BF16)
    wide = keys.astype(F32)
    sums = nn_dot((wide * wide).astype(BF16), head_pick(C, CELL, 0))
    raise_peak(peak_ref, 0, jnp.max(sums, axis=0, keepdims=True))
    raise_peak(peak_ref, 2, jnp.max(jnp.abs(values), axis=0, keepdims=True))
    if q_at is not None:
        queries = nt_dot(w_t[:C, :], normed).astype(BF16)
        q_ref[:, pl.ds(q_at, count)] = queries
        wide = queries.astype(F32)
        sums = nn_dot(head_pick(HEADS, C, 1), (wide * wide).astype(BF16))
        raise_peak(peak_ref, 1, jnp.max(sums, axis=0, keepdims=True))


def turn(qkv_ref, w_ref):
    for at, source in ((0, 0), (C, 2 * C)):
        w_ref[at : at + C, :] = qkv_ref[:, source : source + C].astype(F32).T.astype(BF16)


def attend(windows, pads, k_ref, v_ref, q_ref, m_ref, part, exact, unroll, group):
    def some_heads(first):
        rows = pl.ds(pl.multiple_of(first * HD, HD * group), HD * group)
        half = pl.ds(pl.multiple_of((first // 8) * CELL, CELL), CELL)
        for q_lo, q_n, k_lo, k_n, goes_on, ends in windows:
            q_at = pl.ds(q_lo, q_n)
            lane_head = lax.broadcasted_iota(I32, (CELL, q_n), 0) // HD
            queries = q_ref[half, q_at]
            queries = jnp.concatenate(
                [jnp.where(lane_head == (first + g) % 8, queries, jnp.zeros_like(queries)) for g in range(group)],
                axis=1)
            scores = nn_dot(k_ref[k_lo : k_lo + k_n, half], queries)
            if exact:
                scores = scores - jnp.max(scores, axis=0, keepdims=True)
            weights = jnp.exp2(scores * SCORE_SCALE)
            totals = jnp.sum(jnp.sum(weights.reshape(k_n // 8, 8, group * q_n), axis=0), axis=0, keepdims=True)
            for cell in range(k_n // CELL):
                totals = totals - pads[k_lo // CELL + cell] * weights[cell * CELL : cell * CELL + 1, :]
            mixes = nn_dot(v_ref[rows, k_lo : k_lo + k_n], weights.astype(BF16))
            for g in range(group):
                row = pl.ds(pl.multiple_of((first + g) * HD, HD), HD)
                mixed = mixes[g * HD : (g + 1) * HD, g * q_n : (g + 1) * q_n]
                total = totals[:, g * q_n : (g + 1) * q_n]
                if goes_on:
                    mixed = mixed + part[0][row, q_at]
                    total = total + part[1][pl.ds(first + g, 1), q_at]
                if ends:
                    m_ref[row, q_at] = (mixed / total).astype(BF16)
                else:
                    part[0][row, q_at] = mixed
                    part[1][pl.ds(first + g, 1), q_at] = total

    def step(i, carry):
        for u in range(unroll):
            some_heads((i * unroll + u) * group)
        return carry

    lax.fori_loop(0, HEADS // (unroll * group), step, 0)


def attend_any(plan, whole_windows, pads, peak_ref, k_ref, v_ref, q_ref, m_ref, part):
    bound = peak_ref[0:1, :] * peak_ref[1:2, :] * SCORE_SCALE**2
    off = (bound >= SAFE_EXPONENT * SAFE_EXPONENT) | (peak_ref[2:3, :] >= SAFE_VALUE)
    safe = jnp.max(jnp.where(off, 1.0, 0.0)) < 0.5

    @pl.when(safe)
    def _():
        for windows, unroll, group in plan:
            attend(windows, pads, k_ref, v_ref, q_ref, m_ref, part, False, unroll, group)

    @pl.when(jnp.logical_not(safe))
    def _():
        attend(whole_windows, pads, k_ref, v_ref, q_ref, m_ref, part, True, 1, 1)


def gelu(values):
    return 0.5 * values * (1.0 + lax.erf(values * (2.0**-0.5)))


def finish(rows, mixture_t, gain, offset, out_w, up_w, down_w):
    residual = rows.astype(F32) + nn_dot(mixture_t.astype(F32).T.astype(BF16), out_w)
    residual = residual.astype(BF16).astype(F32)
    normed = norm_rows_of(residual, gain, offset).astype(BF16)
    hidden = gelu(nn_dot(normed, up_w)).astype(BF16)
    return (residual + nn_dot(hidden, down_w)).astype(BF16)


def widest(peak_ref):
    peak_ref[...] = jnp.broadcast_to(jnp.max(peak_ref[...], axis=1, keepdims=True), peak_ref.shape)


def started(*pairs):
    copies = [pltpu.make_async_copy(*pair) for pair in pairs]
    for copy in copies:
        copy.start()
    return copies


def finished(copies):
    for copy in copies:
        copy.wait()


def gather_kernel(
    pos_hbm, count_hbm, x_hbm, norm_hbm, qkv_hbm,
    cells_ref, k_ref, v_ref, q_ref, meta_ref, peak_ref, mixed_ref, total_ref,
    pos_ref, count_ref, x_buf, norm_ref, out_buf, note_out, note_in, qkv_ref, w_ref,
    load_sem, x_sem, send, recv, note_send, note_recv,
):
    me, seq = lax.axis_index("grp"), lax.axis_index("seq")
    x_loads = started(*((x_hbm.at[j], x_buf.at[j], x_sem.at[j]) for j in range(CELLS)))
    loads = started(
        (pos_hbm, pos_ref, load_sem.at[0]), (count_hbm, count_ref, load_sem.at[1]),
        (norm_hbm, norm_ref, load_sem.at[2]), (qkv_hbm.at[0], qkv_ref, load_sem.at[3]),
    )

    hops = (0, 0, 1, 3, 1, 3, 2, 2)
    flips = (0, 1, 0, 0, 1, 1, 0, 1)

    def partner(i):
        return lax.rem(me // 2 + hops[i], CELLS // 2) * 2 + lax.rem(me + flips[i], 2)

    barrier = pltpu.get_barrier_semaphore()
    for i in range(1, CELLS):
        pl.semaphore_signal(barrier, inc=1, device_id=(partner(i), seq), device_id_type=MESH)
    finished(loads[:2])
    finished(x_loads)
    row = lax.broadcasted_iota(I32, (CELLS, CELL), 0)
    for owner in range(CELLS):
        index, place, count = jnp.int32(0), jnp.int32(0), jnp.int32(0)
        for j in range(CELLS):
            position = pos_ref[j]
            mine = position // CELLS == owner
            index = jnp.where(mine, j, index)
            place = jnp.where(mine, position % CELLS, place)
            count = jnp.where(mine, count_ref[j], count)
        out_buf[owner] = x_buf[index]
        note_out[owner] = jnp.where(row == 0, place, count)
    pl.semaphore_wait(barrier, CELLS - 1)

    def sent(i):
        owner = partner(i)
        return (
            pltpu.make_async_remote_copy(
                out_buf.at[owner], cells_ref.at[i], send.at[i], recv.at[i],
                device_id=(owner, seq), device_id_type=MESH),
            pltpu.make_async_remote_copy(
                note_out.at[owner], note_in.at[i], note_send.at[i], note_recv.at[i],
                device_id=(owner, seq), device_id_type=MESH),
        )

    copies = [sent(i) for i in range(1, CELLS)]
    for pair in copies:
        for copy in pair:
            copy.start()
    finished(loads[2:])
    turn(qkv_ref, w_ref)
    gain, offset = norm_ref[0, 0:1, :], norm_ref[0, 1:2, :]
    peak_ref[...] = jnp.zeros_like(peak_ref)

    def take(i):
        for pair in copies[max(i - 1, 0) : i + 1]:
            for copy in pair:
                copy.wait_recv()
        rows, valid = cells_in(
            jnp.concatenate([cells_ref[i], cells_ref[i + 1]], axis=0),
            [note_in[i, 1:2, 0:1], note_in[i + 1, 1:2, 0:1]])
        project(
            rows, valid, gain, offset, w_ref[...], qkv_ref[:, C : 2 * C],
            k_ref, v_ref, q_ref, peak_ref, i * CELL, i * CELL,
        )

    def pads(cells):
        return [(CELL - note_in[i, 1:2, 0:1]).astype(F32) for i in range(cells)]

    cells_ref[0] = out_buf[me]
    note_in[0] = note_out[me]
    part = (mixed_ref, total_ref)
    take(0)
    take(2)
    attend(EARLY, pads(4), k_ref, v_ref, q_ref, None, part, False, 1, 8)
    take(4)
    attend(LATER, pads(6), k_ref, v_ref, q_ref, None, part, False, 1, 8)
    take(6)
    lane = lax.broadcasted_iota(I32, (CELLS, CELL), 1)
    meta = jnp.zeros((CELLS, CELL), I32)
    for j in range(CELLS):
        meta = jnp.where(lane == j, note_in[j], meta)
    meta_ref[...] = meta
    widest(peak_ref)
    for pair in copies:
        for copy in pair:
            copy.wait_send()


def vmem():
    return pl.BlockSpec(memory_space=pltpu.VMEM)


def hbm():
    return pl.BlockSpec(memory_space=pltpu.HBM)


def shape(dims, dtype=BF16):
    return jax.ShapeDtypeStruct(dims, dtype)


def dma(*dims):
    return pltpu.SemaphoreType.DMA(dims)


def gather_cells(pos, counts, cells, norms, qkv):
    return pl.pallas_call(
        gather_kernel,
        out_shape=(
            shape((CELLS, CELL, C)), shape((ROWS, C)), shape((C, ROWS)), shape((C, ROWS)),
            shape((CELLS, CELL), I32), shape((CELLS, CELL), F32), shape((C, HALF), F32), shape((HEADS, HALF), F32),
        ),
        in_specs=[hbm()] * 5,
        out_specs=(vmem(),) * 8,
        scratch_shapes=[
            pltpu.SMEM((CELLS,), I32),
            pltpu.SMEM((CELLS,), I32),
            pltpu.VMEM((CELLS, CELL, C), BF16),
            pltpu.VMEM((2, 4, C), F32),
            pltpu.VMEM((CELLS, CELL, C), BF16),
            pltpu.VMEM((CELLS, CELLS, CELL), I32),
            pltpu.VMEM((CELLS, CELLS, CELL), I32),
            pltpu.VMEM((C, 3 * C), BF16),
            pltpu.VMEM((2 * C, C), BF16),
            dma(4), dma(CELLS), dma(CELLS), dma(CELLS), dma(CELLS), dma(CELLS),
        ],
        compiler_params=pltpu.CompilerParams(
            collective_id=0, has_side_effects=True, vmem_limit_bytes=32 * 2**20),
        name="gather_cells",
    )(pos, counts, cells, norms, qkv)


def aligned_kernel(
    meta_ref, peak_ref, k_ref, v_ref, q_ref, cells_ref, mixed_ref, total_ref, m_ref, placed_ref, count_ref,
    place_ref, mix_ref, sem,
):
    loads = started((meta_ref, place_ref, sem.at[0]))
    pads = [(CELL - meta_ref[1:2, j : j + 1]).astype(F32) for j in range(CELLS)]
    attend_any(((LAST, 1, 8), (OTHERS, 8, 1)), ALIGNED, pads, peak_ref, k_ref, v_ref, q_ref, mix_ref, (mixed_ref, total_ref))
    finished(loads)
    for j in range(CELLS):
        to = place_ref[0, j]
        m_ref[:, pl.ds(pl.multiple_of(to * CELL, CELL), CELL)] = mix_ref[:, j * CELL : (j + 1) * CELL]
        placed_ref[to] = cells_ref[j]
        count_ref[pl.ds(to, 1), :] = jnp.full((1, CELL), place_ref[1, j], I32)


def aligned_attention(meta, peak, keys, values, queries, cells, mixed, total):
    return pl.pallas_call(
        aligned_kernel,
        out_shape=(shape((C, ROWS)), shape((CELLS, CELL, C)), shape((CELLS, CELL), I32)),
        in_specs=[vmem()] * 8,
        out_specs=(vmem(),) * 3,
        scratch_shapes=[
            pltpu.SMEM((CELLS, CELL), I32),
            pltpu.VMEM((C, ROWS), BF16),
            dma(1),
        ],
        compiler_params=pltpu.CompilerParams(vmem_limit_bytes=36 * 2**20),
        name="aligned_attention",
    )(meta, peak, keys, values, queries, cells, mixed, total)


def along(step):
    n_grp, n_seq = lax.axis_size("grp"), lax.axis_size("seq")
    flat = lax.axis_index("grp") * n_seq + lax.axis_index("seq")
    other = lax.rem(flat + step + n_grp * n_seq, n_grp * n_seq)
    return (other // n_seq, lax.rem(other, n_seq))


def middle_kernel(
    note_ref, x_ref, m_ref, norm_ref, qkv_ref, out_ref, up_ref, down_ref,
    y_ref, k_ref, v_ref, q_ref, all_count_ref, peak_ref, mixed_ref, total_ref,
    before_ref, after_ref, note_before, note_after, w_ref,
    send_before, send_after, recv_before, recv_after, note_send, note_recv,
):
    after, before = along(1), along(-1)
    barrier = pltpu.get_barrier_semaphore()
    for device in (after, before):
        pl.semaphore_signal(barrier, inc=1, device_id=device, device_id_type=MESH)
    turn(qkv_ref.at[1], w_ref)
    gain, offset = norm_ref[1, 0:1, :], norm_ref[1, 1:2, :]
    peak_ref[...] = jnp.zeros_like(peak_ref)
    notes = [
        pltpu.make_async_remote_copy(
            note_ref, target, note_send.at[i], note_recv.at[i], device_id=device, device_id_type=MESH)
        for i, (target, device) in enumerate(((note_after, before), (note_before, after)))
    ]

    def to_before(i):
        return pltpu.make_async_remote_copy(
            y_ref.at[pl.ds(i * STEP, STEP)], after_ref.at[pl.ds(i * STEP, STEP)],
            send_before.at[i], recv_after.at[i], device_id=before, device_id_type=MESH)

    def to_after(i):
        return pltpu.make_async_remote_copy(
            y_ref.at[pl.ds(HALF + i * STEP, STEP)], before_ref.at[pl.ds(i * STEP, STEP)],
            send_after.at[i], recv_before.at[i], device_id=after, device_id_type=MESH)

    def place(rows, counts, k_at, q_at):
        rows, valid = cells_in(rows, counts)
        project(
            rows, valid, gain, offset, w_ref[...], qkv_ref[1, :, C : 2 * C],
            k_ref, v_ref, q_ref, peak_ref, k_at, q_at,
        )

    pending = []
    for chunk, copy in ((0, to_before(0)), (2, to_after(0)), (1, to_before(1)), (3, to_after(1))):
        at = chunk * STEP
        y_ref[at : at + STEP, :] = finish(
            jnp.concatenate([x_ref[2 * chunk], x_ref[2 * chunk + 1]], axis=0), m_ref[:, at : at + STEP],
            norm_ref[0, 2:3, :], norm_ref[0, 3:4, :], out_ref[0], up_ref[0], down_ref[0],
        )
        if not pending:
            pl.semaphore_wait(barrier, 2)
            for note in notes:
                note.start()
        else:
            pending[-1].start()
        pending.append(copy)
    own = [note_ref[p : p + 1, 0:1] for p in range(CELLS)]
    place(y_ref[:HALF, :], own[:4], HALF, 0)
    pending[-1].start()
    place(y_ref[HALF:, :], own[4:], ROWS, HALF)
    pads = [None] * 4 + [(CELL - count).astype(F32) for count in own]
    attend(OWN, pads, k_ref, v_ref, q_ref, None, (mixed_ref, total_ref), False, 1, 8)
    for copy in notes:
        copy.wait()
    for incoming, source, note, first, k_first in (
        (to_before, after_ref, note_after, 0, HALF + ROWS), (to_after, before_ref, note_before, 4, 0),
    ):
        for i in range(2):
            incoming(i).wait_recv()
        place(source[...], [note[first + u : first + u + 1, 0:1] for u in range(4)], k_first, None)
    all_count_ref[0:4, :] = note_before[4:8, :]
    all_count_ref[4:12, :] = note_ref[...]
    all_count_ref[12:16, :] = note_after[0:4, :]
    widest(peak_ref)
    for i in range(2):
        to_before(i).wait_send()
        to_after(i).wait_send()


def middle(notes, cells, mixture, norms, qkv, out_w, up_w, down_w):
    return pl.pallas_call(
        middle_kernel,
        out_shape=(
            shape((ROWS, C)), shape((2 * ROWS, C)), shape((C, 2 * ROWS)), shape((C, ROWS)),
            shape((2 * CELLS, CELL), I32), shape((CELLS, CELL), F32), shape((C, ROWS), F32), shape((HEADS, ROWS), F32),
        ),
        in_specs=[vmem()] * 8,
        out_specs=(vmem(),) * 8,
        scratch_shapes=[
            pltpu.VMEM((HALF, C), BF16),
            pltpu.VMEM((HALF, C), BF16),
            pltpu.VMEM((CELLS, CELL), I32),
            pltpu.VMEM((CELLS, CELL), I32),
            pltpu.VMEM((2 * C, C), BF16),
            dma(2), dma(2), dma(2), dma(2), dma(2), dma(2),
        ],
        compiler_params=pltpu.CompilerParams(
            collective_id=1, has_side_effects=True, vmem_limit_bytes=32 * 2**20),
        name="middle",
    )(notes, cells, mixture, norms, qkv, out_w, up_w, down_w)


def shifted_kernel(
    count_ref, peak_ref, k_ref, v_ref, q_ref, mixed_ref, total_ref, x_ref, norm_ref, out_ref, up_ref, down_ref,
    y_hbm, m_ref, y_ref, store_sem,
):
    pads = [(CELL - count_ref[j : j + 1, 0:1]).astype(F32) for j in range(2 * CELLS)]
    attend_any(((BORROWED, 2, 4),), SHIFTED, pads, peak_ref, k_ref, v_ref, q_ref, m_ref, (mixed_ref, total_ref))
    stores = []
    for i in range(ROWS // HALF):
        at = i * HALF
        done = finish(
            x_ref[at : at + HALF, :], m_ref[:, at : at + HALF], norm_ref[1, 2:3, :], norm_ref[1, 3:4, :],
            out_ref[1], up_ref[1], down_ref[1],
        )
        for u in range(4):
            cell = CELLS // 2 + 4 * i + u
            keep = lax.broadcasted_iota(I32, (CELL, 1), 0) < count_ref[cell : cell + 1, 0:1]
            part = done[u * CELL : (u + 1) * CELL, :]
            y_ref[at + u * CELL : at + (u + 1) * CELL, :] = jnp.where(keep, part, jnp.zeros_like(part))
        rows = pl.ds(at, HALF)
        stores += started((y_ref.at[rows], y_hbm.at[rows], store_sem.at[i]))
    finished(stores)


def shifted_block(counts, peak, keys, values, queries, mixed, total, rows, norms, out_w, up_w, down_w):
    return pl.pallas_call(
        shifted_kernel,
        out_shape=shape((ROWS, C)),
        in_specs=[vmem()] * 12,
        out_specs=hbm(),
        scratch_shapes=[
            pltpu.VMEM((C, ROWS), BF16),
            pltpu.VMEM((ROWS, C), BF16),
            dma(4),
        ],
        compiler_params=pltpu.CompilerParams(vmem_limit_bytes=36 * 2**20),
        name="shifted_block",
    )(counts, peak, keys, values, queries, mixed, total, rows, norms, out_w, up_w, down_w)


def body(points, hilbert_pos, valid_counts, norms, qkv, out_w, up_w, down_w):
    cells, keys, values, queries, meta, peak, mixed, total = gather_cells(*(
        pltpu.with_memory_space_constraint(array, pltpu.HBM)
        for array in (hilbert_pos, valid_counts, points.reshape(CELLS, CELL, C), norms, qkv)))
    mixture, placed, notes = aligned_attention(meta, peak, keys, values, queries, cells, mixed, total)
    rows, keys, values, queries, counts, peak, mixed, total = middle(notes, placed, mixture, norms, qkv, out_w, up_w, down_w)
    return shifted_block(
        counts, peak, keys, values, queries, mixed, total, rows, norms, out_w, up_w, down_w)


def solution(mesh):
    return jax.shard_map(
        body,
        mesh=mesh,
        in_specs=(
            P(("grp", "seq"), None), P(("grp", "seq")), P(("grp", "seq")), P(), P(), P(), P(), P(),
        ),
        out_specs=P(("grp", "seq"), None),
        check_vma=False,
    )
```

```python
import math

import jax
import jax.numpy as jnp
from jax import lax
from jax.experimental import pallas as pl
from jax.experimental.pallas import tpu as pltpu
from jax.sharding import PartitionSpec as P

C = 256
HEADS = 16
HD = 16
HID = 1024
CELL = 128
CELLS = 8
ROWS = CELL * CELLS
HALF = ROWS // 2
STEP = 2 * CELL
F32 = jnp.float32
BF16 = jnp.bfloat16
I32 = jnp.int32
MESH = pl.DeviceIdType.MESH
SCORE_SCALE = HD**-0.5 * math.log2(math.e)
SAFE_EXPONENT = 60.0
SAFE_VALUE = 2.0**40
EARLY = ((0, HALF, 0, HALF, False, False),)
LATER = ((0, HALF, HALF, STEP, True, False),)
LAST = ((0, HALF, HALF + STEP, STEP, True, True),)
OTHERS = ((HALF, HALF, 0, ROWS, False, True),)
ALIGNED = ((0, HALF, 0, ROWS, False, True), (HALF, HALF, 0, ROWS, False, True))
OWN = ((0, HALF, HALF, HALF, False, False), (HALF, HALF, ROWS, HALF, False, False))
AFTER = ((HALF, HALF, ROWS + HALF, HALF, True, False),)
BEFORE = ((0, HALF, 0, STEP, True, False),)
BORROWED = ((0, HALF, STEP, STEP, True, True),)
SHIFTED = ((0, HALF, 0, ROWS, False, True), (HALF, HALF, ROWS, ROWS, False, True))


def nt_dot(a, b):
    return lax.dot_general(a, b, (((1,), (1,)), ((), ())), preferred_element_type=F32)


def nn_dot(a, b):
    return jnp.dot(a, b, preferred_element_type=F32)


def norm_rows_of(values, gain, offset):
    center = jnp.mean(values, axis=-1, keepdims=True)
    spread = values - center
    second = jnp.mean(spread * spread, axis=-1, keepdims=True)
    return spread * lax.rsqrt(second + 1e-5) * gain + offset


def head_pick(rows, columns, channel_axis):
    channel = lax.broadcasted_iota(I32, (rows, columns), channel_axis) // HD
    head = lax.broadcasted_iota(I32, (rows, columns), 1 - channel_axis)
    return jnp.where(channel == head, 1.0, 0.0).astype(BF16)


def first_valid(rows, count):
    index = lax.broadcasted_iota(I32, (CELL, 1), 0)
    return jnp.where(index < count, rows, rows[0:1, :])


def lane_valid(count):
    return jnp.where(lax.broadcasted_iota(I32, (1, CELL), 1) < count, 1.0, 0.0)


def raise_peak(peak_ref, row, tall):
    peak = peak_ref[row : row + 1, :]
    for at in range(0, tall.shape[1], CELL):
        peak = jnp.maximum(peak, tall[:, at : at + CELL])
    peak_ref[row : row + 1, :] = peak


def cells_in(rows, counts):
    wide = rows.astype(F32)
    cells = [first_valid(wide[u * CELL : (u + 1) * CELL], count) for u, count in enumerate(counts)]
    return jnp.concatenate(cells, axis=0), jnp.concatenate([lane_valid(count) for count in counts], axis=1)


def project(rows, valid, gain, offset, w_t, w_k, k_ref, v_ref, q_ref, peak_ref, k_at, q_at):
    count = rows.shape[0]
    normed = norm_rows_of(rows, gain, offset).astype(BF16)
    keys = nn_dot(normed, w_k).astype(BF16)
    k_ref[pl.ds(k_at, count), :] = keys
    values = nt_dot(w_t[C:, :], normed) * valid
    v_ref[:, pl.ds(k_at, count)] = values.astype(BF16)
    wide = keys.astype(F32)
    sums = nn_dot((wide * wide).astype(BF16), head_pick(C, CELL, 0))
    raise_peak(peak_ref, 0, jnp.max(sums, axis=0, keepdims=True))
    raise_peak(peak_ref, 2, jnp.max(jnp.abs(values), axis=0, keepdims=True))
    if q_at is not None:
        queries = nt_dot(w_t[:C, :], normed).astype(BF16)
        q_ref[:, pl.ds(q_at, count)] = queries
        wide = queries.astype(F32)
        sums = nn_dot(head_pick(HEADS, C, 1), (wide * wide).astype(BF16))
        raise_peak(peak_ref, 1, jnp.max(sums, axis=0, keepdims=True))


def turn(qkv_ref, w_ref):
    for at, source in ((0, 0), (C, 2 * C)):
        w_ref[at : at + C, :] = qkv_ref[:, source : source + C].astype(F32).T.astype(BF16)


def attend(windows, pads, k_ref, v_ref, q_ref, m_ref, part, exact, unroll, group):
    def some_heads(first):
        rows = pl.ds(pl.multiple_of(first * HD, HD * group), HD * group)
        half = pl.ds(pl.multiple_of((first // 8) * CELL, CELL), CELL)
        for q_lo, q_n, k_lo, k_n, goes_on, ends in windows:
            q_at = pl.ds(q_lo, q_n)
            lane_head = lax.broadcasted_iota(I32, (CELL, q_n), 0) // HD
            queries = q_ref[half, q_at]
            queries = jnp.concatenate(
                [jnp.where(lane_head == (first + g) % 8, queries, jnp.zeros_like(queries)) for g in range(group)],
                axis=1)
            scores = nn_dot(k_ref[k_lo : k_lo + k_n, half], queries)
            if exact:
                scores = scores - jnp.max(scores, axis=0, keepdims=True)
            weights = jnp.exp2(scores * SCORE_SCALE)
            totals = jnp.sum(jnp.sum(weights.reshape(k_n // 8, 8, group * q_n), axis=0), axis=0, keepdims=True)
            for cell in range(k_n // CELL):
                totals = totals - pads[k_lo // CELL + cell] * weights[cell * CELL : cell * CELL + 1, :]
            mixes = nn_dot(v_ref[rows, k_lo : k_lo + k_n], weights.astype(BF16))
            for g in range(group):
                row = pl.ds(pl.multiple_of((first + g) * HD, HD), HD)
                mixed = mixes[g * HD : (g + 1) * HD, g * q_n : (g + 1) * q_n]
                total = totals[:, g * q_n : (g + 1) * q_n]
                if goes_on:
                    mixed = mixed + part[0][row, q_at]
                    total = total + part[1][pl.ds(first + g, 1), q_at]
                if ends:
                    m_ref[row, q_at] = (mixed / total).astype(BF16)
                else:
                    part[0][row, q_at] = mixed
                    part[1][pl.ds(first + g, 1), q_at] = total

    def step(i, carry):
        for u in range(unroll):
            some_heads((i * unroll + u) * group)
        return carry

    lax.fori_loop(0, HEADS // (unroll * group), step, 0)


def attend_any(plan, whole_windows, settled, pads, peak_ref, k_ref, v_ref, q_ref, m_ref, part):
    bound = peak_ref[0:1, :] * peak_ref[1:2, :] * SCORE_SCALE**2
    off = (bound >= SAFE_EXPONENT * SAFE_EXPONENT) | (peak_ref[2:3, :] >= SAFE_VALUE)
    safe = jnp.max(jnp.where(off, 1.0, 0.0)) < 0.5

    @pl.when(safe)
    def _():
        for windows, unroll, group in plan:
            attend(windows, pads, k_ref, v_ref, q_ref, m_ref, part, False, unroll, group)
        for head in range(HEADS if settled is not None else 0):
            row = slice(head * HD, (head + 1) * HD)
            m_ref[row, settled:] = (part[0][row, settled:] / part[1][head : head + 1, settled:]).astype(BF16)

    @pl.when(jnp.logical_not(safe))
    def _():
        attend(whole_windows, pads, k_ref, v_ref, q_ref, m_ref, part, True, 1, 1)


def gelu(values):
    return 0.5 * values * (1.0 + lax.erf(values * (2.0**-0.5)))


def finish(rows, mixture_t, gain, offset, out_w, up_w, down_w):
    residual = rows.astype(F32) + nn_dot(mixture_t.astype(F32).T.astype(BF16), out_w)
    residual = residual.astype(BF16).astype(F32)
    normed = norm_rows_of(residual, gain, offset).astype(BF16)
    hidden = gelu(nn_dot(normed, up_w)).astype(BF16)
    return (residual + nn_dot(hidden, down_w)).astype(BF16)


def widest(peak_ref):
    peak_ref[...] = jnp.broadcast_to(jnp.max(peak_ref[...], axis=1, keepdims=True), peak_ref.shape)


def started(*pairs):
    copies = [pltpu.make_async_copy(*pair) for pair in pairs]
    for copy in copies:
        copy.start()
    return copies


def finished(copies):
    for copy in copies:
        copy.wait()


def gather_kernel(
    pos_hbm, count_hbm, x_hbm, norm_hbm, qkv_hbm,
    cells_ref, k_ref, v_ref, q_ref, meta_ref, peak_ref, mixed_ref, total_ref,
    pos_ref, count_ref, x_buf, norm_ref, out_buf, note_out, note_in, qkv_ref, w_ref,
    load_sem, x_sem, send, recv, note_send, note_recv,
):
    me, seq = lax.axis_index("grp"), lax.axis_index("seq")
    x_loads = started(*((x_hbm.at[j], x_buf.at[j], x_sem.at[j]) for j in range(CELLS)))
    loads = started(
        (pos_hbm, pos_ref, load_sem.at[0]), (count_hbm, count_ref, load_sem.at[1]),
        (norm_hbm, norm_ref, load_sem.at[2]), (qkv_hbm.at[0], qkv_ref, load_sem.at[3]),
    )

    hops = (0, 0, 1, 3, 1, 3, 2, 2)
    flips = (0, 1, 0, 0, 1, 1, 0, 1)

    def partner(i):
        return lax.rem(me // 2 + hops[i], CELLS // 2) * 2 + lax.rem(me + flips[i], 2)

    barrier = pltpu.get_barrier_semaphore()
    for i in range(1, CELLS):
        pl.semaphore_signal(barrier, inc=1, device_id=(partner(i), seq), device_id_type=MESH)
    finished(loads[:2])
    finished(x_loads)
    row = lax.broadcasted_iota(I32, (CELLS, CELL), 0)
    for owner in range(CELLS):
        index, place, count = jnp.int32(0), jnp.int32(0), jnp.int32(0)
        for j in range(CELLS):
            position = pos_ref[j]
            mine = position // CELLS == owner
            index = jnp.where(mine, j, index)
            place = jnp.where(mine, position % CELLS, place)
            count = jnp.where(mine, count_ref[j], count)
        out_buf[owner] = x_buf[index]
        note_out[owner] = jnp.where(row == 0, place, count)
    pl.semaphore_wait(barrier, CELLS - 1)

    def sent(i):
        owner = partner(i)
        return (
            pltpu.make_async_remote_copy(
                out_buf.at[owner], cells_ref.at[i], send.at[i], recv.at[i],
                device_id=(owner, seq), device_id_type=MESH),
            pltpu.make_async_remote_copy(
                note_out.at[owner], note_in.at[i], note_send.at[i], note_recv.at[i],
                device_id=(owner, seq), device_id_type=MESH),
        )

    copies = [sent(i) for i in range(1, CELLS)]
    for pair in copies:
        for copy in pair:
            copy.start()
    finished(loads[2:])
    turn(qkv_ref, w_ref)
    gain, offset = norm_ref[0, 0:1, :], norm_ref[0, 1:2, :]
    peak_ref[...] = jnp.zeros_like(peak_ref)

    def take(i):
        for pair in copies[max(i - 1, 0) : i + 1]:
            for copy in pair:
                copy.wait_recv()
        rows, valid = cells_in(
            jnp.concatenate([cells_ref[i], cells_ref[i + 1]], axis=0),
            [note_in[i, 1:2, 0:1], note_in[i + 1, 1:2, 0:1]])
        project(
            rows, valid, gain, offset, w_ref[...], qkv_ref[:, C : 2 * C],
            k_ref, v_ref, q_ref, peak_ref, i * CELL, i * CELL,
        )

    def pads(cells):
        return [(CELL - note_in[i, 1:2, 0:1]).astype(F32) for i in range(cells)]

    cells_ref[0] = out_buf[me]
    note_in[0] = note_out[me]
    part = (mixed_ref, total_ref)
    take(0)
    take(2)
    attend(EARLY, pads(4), k_ref, v_ref, q_ref, None, part, False, 1, 8)
    take(4)
    attend(LATER, pads(6), k_ref, v_ref, q_ref, None, part, False, 1, 8)
    take(6)
    lane = lax.broadcasted_iota(I32, (CELLS, CELL), 1)
    meta = jnp.zeros((CELLS, CELL), I32)
    for j in range(CELLS):
        meta = jnp.where(lane == j, note_in[j], meta)
    meta_ref[...] = meta
    widest(peak_ref)
    for pair in copies:
        for copy in pair:
            copy.wait_send()


def vmem():
    return pl.BlockSpec(memory_space=pltpu.VMEM)


def hbm():
    return pl.BlockSpec(memory_space=pltpu.HBM)


def shape(dims, dtype=BF16):
    return jax.ShapeDtypeStruct(dims, dtype)


def dma(*dims):
    return pltpu.SemaphoreType.DMA(dims)


def gather_cells(pos, counts, cells, norms, qkv):
    return pl.pallas_call(
        gather_kernel,
        out_shape=(
            shape((CELLS, CELL, C)), shape((ROWS, C)), shape((C, ROWS)), shape((C, ROWS)),
            shape((CELLS, CELL), I32), shape((CELLS, CELL), F32), shape((C, HALF), F32), shape((HEADS, HALF), F32),
        ),
        in_specs=[hbm()] * 5,
        out_specs=(vmem(),) * 8,
        scratch_shapes=[
            pltpu.SMEM((CELLS,), I32),
            pltpu.SMEM((CELLS,), I32),
            pltpu.VMEM((CELLS, CELL, C), BF16),
            pltpu.VMEM((2, 4, C), F32),
            pltpu.VMEM((CELLS, CELL, C), BF16),
            pltpu.VMEM((CELLS, CELLS, CELL), I32),
            pltpu.VMEM((CELLS, CELLS, CELL), I32),
            pltpu.VMEM((C, 3 * C), BF16),
            pltpu.VMEM((2 * C, C), BF16),
            dma(4), dma(CELLS), dma(CELLS), dma(CELLS), dma(CELLS), dma(CELLS),
        ],
        compiler_params=pltpu.CompilerParams(
            collective_id=0, has_side_effects=True, vmem_limit_bytes=32 * 2**20),
        name="gather_cells",
    )(pos, counts, cells, norms, qkv)


def aligned_kernel(
    meta_ref, peak_ref, k_ref, v_ref, q_ref, cells_ref, mixed_ref, total_ref, m_ref, placed_ref, count_ref,
    place_ref, mix_ref, sem,
):
    loads = started((meta_ref, place_ref, sem.at[0]))
    pads = [(CELL - meta_ref[1:2, j : j + 1]).astype(F32) for j in range(CELLS)]
    attend_any(((LAST, 1, 8), (OTHERS, 8, 1)), ALIGNED, None, pads, peak_ref, k_ref, v_ref, q_ref, mix_ref, (mixed_ref, total_ref))
    finished(loads)
    for j in range(CELLS):
        to = place_ref[0, j]
        m_ref[:, pl.ds(pl.multiple_of(to * CELL, CELL), CELL)] = mix_ref[:, j * CELL : (j + 1) * CELL]
        placed_ref[to] = cells_ref[j]
        count_ref[pl.ds(to, 1), :] = jnp.full((1, CELL), place_ref[1, j], I32)


def aligned_attention(meta, peak, keys, values, queries, cells, mixed, total):
    return pl.pallas_call(
        aligned_kernel,
        out_shape=(shape((C, ROWS)), shape((CELLS, CELL, C)), shape((CELLS, CELL), I32)),
        in_specs=[vmem()] * 8,
        out_specs=(vmem(),) * 3,
        scratch_shapes=[
            pltpu.SMEM((CELLS, CELL), I32),
            pltpu.VMEM((C, ROWS), BF16),
            dma(1),
        ],
        compiler_params=pltpu.CompilerParams(vmem_limit_bytes=36 * 2**20),
        name="aligned_attention",
    )(meta, peak, keys, values, queries, cells, mixed, total)


def along(step):
    n_grp, n_seq = lax.axis_size("grp"), lax.axis_size("seq")
    flat = lax.axis_index("grp") * n_seq + lax.axis_index("seq")
    other = lax.rem(flat + step + n_grp * n_seq, n_grp * n_seq)
    return (other // n_seq, lax.rem(other, n_seq))


def middle_kernel(
    note_ref, x_ref, m_ref, norm_ref, qkv_ref, out_ref, up_ref, down_ref,
    y_ref, k_ref, v_ref, q_ref, all_count_ref, peak_ref, mixed_ref, total_ref,
    before_ref, after_ref, note_before, note_after, w_ref,
    send_before, send_after, recv_before, recv_after, note_send, note_recv,
):
    after, before = along(1), along(-1)
    barrier = pltpu.get_barrier_semaphore()
    for device in (after, before):
        pl.semaphore_signal(barrier, inc=1, device_id=device, device_id_type=MESH)
    turn(qkv_ref.at[1], w_ref)
    gain, offset = norm_ref[1, 0:1, :], norm_ref[1, 1:2, :]
    peak_ref[...] = jnp.zeros_like(peak_ref)
    notes = [
        pltpu.make_async_remote_copy(
            note_ref, target, note_send.at[i], note_recv.at[i], device_id=device, device_id_type=MESH)
        for i, (target, device) in enumerate(((note_after, before), (note_before, after)))
    ]

    def to_before(i):
        return pltpu.make_async_remote_copy(
            y_ref.at[pl.ds(i * STEP, STEP)], after_ref.at[pl.ds(i * STEP, STEP)],
            send_before.at[i], recv_after.at[i], device_id=before, device_id_type=MESH)

    def to_after(i):
        return pltpu.make_async_remote_copy(
            y_ref.at[pl.ds(HALF + i * STEP, STEP)], before_ref.at[pl.ds(i * STEP, STEP)],
            send_after.at[i], recv_before.at[i], device_id=after, device_id_type=MESH)

    def place(rows, counts, k_at, q_at):
        rows, valid = cells_in(rows, counts)
        project(
            rows, valid, gain, offset, w_ref[...], qkv_ref[1, :, C : 2 * C],
            k_ref, v_ref, q_ref, peak_ref, k_at, q_at,
        )

    for chunk in (2, 3, 0, 1):
        at = chunk * STEP
        y_ref[at : at + STEP, :] = finish(
            jnp.concatenate([x_ref[2 * chunk], x_ref[2 * chunk + 1]], axis=0), m_ref[:, at : at + STEP],
            norm_ref[0, 2:3, :], norm_ref[0, 3:4, :], out_ref[0], up_ref[0], down_ref[0],
        )
    pl.semaphore_wait(barrier, 2)
    for copy in notes + [to_after(0), to_after(1), to_before(0)]:
        copy.start()
    own = [note_ref[p : p + 1, 0:1] for p in range(CELLS)]
    place(y_ref[HALF:, :], own[4:], ROWS, HALF)
    to_before(1).start()
    place(y_ref[:HALF, :], own[:4], HALF, 0)
    part = (mixed_ref, total_ref)
    pads = [None] * 4 + [(CELL - count).astype(F32) for count in own]
    attend(OWN, pads, k_ref, v_ref, q_ref, None, part, False, 1, 8)
    for copy in notes:
        copy.wait()
    before_counts = [note_before[p : p + 1, 0:1] for p in range(4, 8)]
    after_counts = [note_after[p : p + 1, 0:1] for p in range(4)]
    pads = [(CELL - count).astype(F32) for count in before_counts + own + after_counts]
    for i in range(2):
        to_before(i).wait_recv()
    place(after_ref[...], after_counts, HALF + ROWS, None)
    attend(AFTER, pads, k_ref, v_ref, q_ref, None, part, False, 1, 8)
    to_after(0).wait_recv()
    place(before_ref[:STEP, :], before_counts[:2], 0, None)
    attend(BEFORE, pads, k_ref, v_ref, q_ref, None, part, False, 1, 8)
    to_after(1).wait_recv()
    place(before_ref[STEP:, :], before_counts[2:], STEP, None)
    all_count_ref[0:4, :] = note_before[4:8, :]
    all_count_ref[4:12, :] = note_ref[...]
    all_count_ref[12:16, :] = note_after[0:4, :]
    widest(peak_ref)
    for i in range(2):
        to_before(i).wait_send()
        to_after(i).wait_send()


def middle(notes, cells, mixture, norms, qkv, out_w, up_w, down_w):
    return pl.pallas_call(
        middle_kernel,
        out_shape=(
            shape((ROWS, C)), shape((2 * ROWS, C)), shape((C, 2 * ROWS)), shape((C, ROWS)),
            shape((2 * CELLS, CELL), I32), shape((CELLS, CELL), F32), shape((C, ROWS), F32), shape((HEADS, ROWS), F32),
        ),
        in_specs=[vmem()] * 8,
        out_specs=(vmem(),) * 8,
        scratch_shapes=[
            pltpu.VMEM((HALF, C), BF16),
            pltpu.VMEM((HALF, C), BF16),
            pltpu.VMEM((CELLS, CELL), I32),
            pltpu.VMEM((CELLS, CELL), I32),
            pltpu.VMEM((2 * C, C), BF16),
            dma(2), dma(2), dma(2), dma(2), dma(2), dma(2),
        ],
        compiler_params=pltpu.CompilerParams(
            collective_id=1, has_side_effects=True, vmem_limit_bytes=32 * 2**20),
        name="middle",
    )(notes, cells, mixture, norms, qkv, out_w, up_w, down_w)


def shifted_kernel(
    count_ref, peak_ref, k_ref, v_ref, q_ref, mixed_ref, total_ref, x_ref, norm_ref, out_ref, up_ref, down_ref,
    y_hbm, m_ref, y_ref, store_sem,
):
    pads = [(CELL - count_ref[j : j + 1, 0:1]).astype(F32) for j in range(2 * CELLS)]
    attend_any(((BORROWED, 1, 8),), SHIFTED, HALF, pads, peak_ref, k_ref, v_ref, q_ref, m_ref, (mixed_ref, total_ref))
    stores = []
    for i in range(ROWS // HALF):
        at = i * HALF
        done = finish(
            x_ref[at : at + HALF, :], m_ref[:, at : at + HALF], norm_ref[1, 2:3, :], norm_ref[1, 3:4, :],
            out_ref[1], up_ref[1], down_ref[1],
        )
        for u in range(4):
            cell = CELLS // 2 + 4 * i + u
            keep = lax.broadcasted_iota(I32, (CELL, 1), 0) < count_ref[cell : cell + 1, 0:1]
            part = done[u * CELL : (u + 1) * CELL, :]
            y_ref[at + u * CELL : at + (u + 1) * CELL, :] = jnp.where(keep, part, jnp.zeros_like(part))
        rows = pl.ds(at, HALF)
        stores += started((y_ref.at[rows], y_hbm.at[rows], store_sem.at[i]))
    finished(stores)


def shifted_block(counts, peak, keys, values, queries, mixed, total, rows, norms, out_w, up_w, down_w):
    return pl.pallas_call(
        shifted_kernel,
        out_shape=shape((ROWS, C)),
        in_specs=[vmem()] * 12,
        out_specs=hbm(),
        scratch_shapes=[
            pltpu.VMEM((C, ROWS), BF16),
            pltpu.VMEM((ROWS, C), BF16),
            dma(4),
        ],
        compiler_params=pltpu.CompilerParams(vmem_limit_bytes=36 * 2**20),
        name="shifted_block",
    )(counts, peak, keys, values, queries, mixed, total, rows, norms, out_w, up_w, down_w)


def body(points, hilbert_pos, valid_counts, norms, qkv, out_w, up_w, down_w):
    cells, keys, values, queries, meta, peak, mixed, total = gather_cells(*(
        pltpu.with_memory_space_constraint(array, pltpu.HBM)
        for array in (hilbert_pos, valid_counts, points.reshape(CELLS, CELL, C), norms, qkv)))
    mixture, placed, notes = aligned_attention(meta, peak, keys, values, queries, cells, mixed, total)
    rows, keys, values, queries, counts, peak, mixed, total = middle(notes, placed, mixture, norms, qkv, out_w, up_w, down_w)
    return shifted_block(
        counts, peak, keys, values, queries, mixed, total, rows, norms, out_w, up_w, down_w)


def solution(mesh):
    return jax.shard_map(
        body,
        mesh=mesh,
        in_specs=(
            P(("grp", "seq"), None), P(("grp", "seq")), P(("grp", "seq")), P(), P(), P(), P(), P(),
        ),
        out_specs=P(("grp", "seq"), None),
        check_vma=False,
    )
```

```python
import math

import jax
import jax.numpy as jnp
from jax import lax
from jax.experimental import pallas as pl
from jax.experimental.pallas import tpu as pltpu
from jax.sharding import PartitionSpec as P

C = 256
HEADS = 16
HD = 16
HID = 1024
CELL = 128
CELLS = 8
ROWS = CELL * CELLS
HALF = ROWS // 2
STEP = 2 * CELL
F32 = jnp.float32
BF16 = jnp.bfloat16
I32 = jnp.int32
MESH = pl.DeviceIdType.MESH
SCORE_SCALE = HD**-0.5 * math.log2(math.e)
SAFE_EXPONENT = 60.0
SAFE_VALUE = 2.0**40
EARLY = ((0, HALF, 0, HALF, False, False),)
LATER = ((0, HALF, HALF, STEP, True, False),)
LAST = ((0, HALF, HALF + STEP, STEP, True, True),)
OTHERS = ((HALF, HALF, 0, ROWS, False, True),)
ALIGNED = ((0, HALF, 0, ROWS, False, True), (HALF, HALF, 0, ROWS, False, True))
OWN = ((0, HALF, HALF, HALF, False, False), (HALF, HALF, ROWS, HALF, False, False))
AFTER = ((HALF, HALF, ROWS + HALF, HALF, True, False),)
BEFORE = ((0, HALF, 0, STEP, True, False),)
BORROWED = ((0, HALF, STEP, STEP, True, True),)
SHIFTED = ((0, HALF, 0, ROWS, False, True), (HALF, HALF, ROWS, ROWS, False, True))


def nt_dot(a, b):
    return lax.dot_general(a, b, (((1,), (1,)), ((), ())), preferred_element_type=F32)


def nn_dot(a, b):
    return jnp.dot(a, b, preferred_element_type=F32)


def norm_rows_of(values, gain, offset):
    center = jnp.mean(values, axis=-1, keepdims=True)
    spread = values - center
    second = jnp.mean(spread * spread, axis=-1, keepdims=True)
    return spread * lax.rsqrt(second + 1e-5) * gain + offset


def head_pick(rows, columns, channel_axis):
    channel = lax.broadcasted_iota(I32, (rows, columns), channel_axis) // HD
    head = lax.broadcasted_iota(I32, (rows, columns), 1 - channel_axis)
    return jnp.where(channel == head, 1.0, 0.0).astype(BF16)


def first_valid(rows, count):
    index = lax.broadcasted_iota(I32, (CELL, 1), 0)
    return jnp.where(index < count, rows, rows[0:1, :])


def lane_valid(count):
    return jnp.where(lax.broadcasted_iota(I32, (1, CELL), 1) < count, 1.0, 0.0)


def raise_peak(peak_ref, row, tall):
    peak = peak_ref[row : row + 1, :]
    for at in range(0, tall.shape[1], CELL):
        peak = jnp.maximum(peak, tall[:, at : at + CELL])
    peak_ref[row : row + 1, :] = peak


def cells_in(rows, counts):
    wide = rows.astype(F32)
    cells = [first_valid(wide[u * CELL : (u + 1) * CELL], count) for u, count in enumerate(counts)]
    return jnp.concatenate(cells, axis=0), jnp.concatenate([lane_valid(count) for count in counts], axis=1)


def project(rows, valid, gain, offset, w_t, w_k, k_ref, v_ref, q_ref, peak_ref, k_at, q_at):
    count = rows.shape[0]
    normed = norm_rows_of(rows, gain, offset).astype(BF16)
    keys = nn_dot(normed, w_k).astype(BF16)
    k_ref[pl.ds(k_at, count), :] = keys
    values = nt_dot(w_t[C:, :], normed) * valid
    v_ref[:, pl.ds(k_at, count)] = values.astype(BF16)
    wide = keys.astype(F32)
    sums = nn_dot((wide * wide).astype(BF16), head_pick(C, CELL, 0))
    raise_peak(peak_ref, 0, jnp.max(sums, axis=0, keepdims=True))
    raise_peak(peak_ref, 2, jnp.max(jnp.abs(values), axis=0, keepdims=True))
    if q_at is not None:
        queries = nt_dot(w_t[:C, :], normed).astype(BF16)
        q_ref[:, pl.ds(q_at, count)] = queries
        wide = queries.astype(F32)
        sums = nn_dot(head_pick(HEADS, C, 1), (wide * wide).astype(BF16))
        raise_peak(peak_ref, 1, jnp.max(sums, axis=0, keepdims=True))


def turn(qkv_ref, w_ref):
    for at, source in ((0, 0), (C, 2 * C)):
        w_ref[at : at + C, :] = qkv_ref[:, source : source + C].astype(F32).T.astype(BF16)


def attend(windows, pads, k_ref, v_ref, q_ref, m_ref, part, exact, unroll, group):
    def some_heads(first):
        rows = pl.ds(pl.multiple_of(first * HD, HD * group), HD * group)
        half = pl.ds(pl.multiple_of((first // 8) * CELL, CELL), CELL)
        for q_lo, q_n, k_lo, k_n, goes_on, ends in windows:
            q_at = pl.ds(q_lo, q_n)
            lane_head = lax.broadcasted_iota(I32, (CELL, q_n), 0) // HD
            queries = q_ref[half, q_at]
            queries = jnp.concatenate(
                [jnp.where(lane_head == (first + g) % 8, queries, jnp.zeros_like(queries)) for g in range(group)],
                axis=1)
            scores = nn_dot(k_ref[k_lo : k_lo + k_n, half], queries)
            if exact:
                scores = scores - jnp.max(scores, axis=0, keepdims=True)
            weights = jnp.exp2(scores * SCORE_SCALE)
            totals = jnp.sum(jnp.sum(weights.reshape(k_n // 8, 8, group * q_n), axis=0), axis=0, keepdims=True)
            for cell in range(k_n // CELL):
                totals = totals - pads[k_lo // CELL + cell] * weights[cell * CELL : cell * CELL + 1, :]
            mixes = nn_dot(v_ref[rows, k_lo : k_lo + k_n], weights.astype(BF16))
            for g in range(group):
                row = pl.ds(pl.multiple_of((first + g) * HD, HD), HD)
                mixed = mixes[g * HD : (g + 1) * HD, g * q_n : (g + 1) * q_n]
                total = totals[:, g * q_n : (g + 1) * q_n]
                if goes_on:
                    mixed = mixed + part[0][row, q_at]
                    total = total + part[1][pl.ds(first + g, 1), q_at]
                if ends:
                    m_ref[row, q_at] = (mixed / total).astype(BF16)
                else:
                    part[0][row, q_at] = mixed
                    part[1][pl.ds(first + g, 1), q_at] = total

    def step(i, carry):
        for u in range(unroll):
            some_heads((i * unroll + u) * group)
        return carry

    lax.fori_loop(0, HEADS // (unroll * group), step, 0)


def attend_any(plan, whole_windows, settled, pads, peak_ref, k_ref, v_ref, q_ref, m_ref, part):
    bound = peak_ref[0:1, :] * peak_ref[1:2, :] * SCORE_SCALE**2
    off = (bound >= SAFE_EXPONENT * SAFE_EXPONENT) | (peak_ref[2:3, :] >= SAFE_VALUE)
    safe = jnp.max(jnp.where(off, 1.0, 0.0)) < 0.5

    @pl.when(safe)
    def _():
        for windows, unroll, group in plan:
            attend(windows, pads, k_ref, v_ref, q_ref, m_ref, part, False, unroll, group)
        for head in range(HEADS if settled is not None else 0):
            row = slice(head * HD, (head + 1) * HD)
            m_ref[row, settled:] = (part[0][row, settled:] / part[1][head : head + 1, settled:]).astype(BF16)

    @pl.when(jnp.logical_not(safe))
    def _():
        attend(whole_windows, pads, k_ref, v_ref, q_ref, m_ref, part, True, 1, 1)


def gelu(values):
    return 0.5 * values * (1.0 + lax.erf(values * (2.0**-0.5)))


def finish(rows, mixture_t, gain, offset, out_w, up_w, down_w):
    residual = rows.astype(F32) + nn_dot(mixture_t.astype(F32).T.astype(BF16), out_w)
    residual = residual.astype(BF16).astype(F32)
    normed = norm_rows_of(residual, gain, offset).astype(BF16)
    hidden = gelu(nn_dot(normed, up_w)).astype(BF16)
    return (residual + nn_dot(hidden, down_w)).astype(BF16)


def widest(peak_ref):
    peak_ref[...] = jnp.broadcast_to(jnp.max(peak_ref[...], axis=1, keepdims=True), peak_ref.shape)


def started(*pairs):
    copies = [pltpu.make_async_copy(*pair) for pair in pairs]
    for copy in copies:
        copy.start()
    return copies


def finished(copies):
    for copy in copies:
        copy.wait()


def gather_kernel(
    pos_hbm, count_hbm, x_hbm, norm_hbm, qkv_hbm,
    cells_ref, k_ref, v_ref, q_ref, meta_ref, peak_ref, mixed_ref, total_ref,
    pos_ref, count_ref, x_buf, norm_ref, out_buf, note_out, note_in, qkv_ref, w_ref,
    load_sem, x_sem, send, recv, note_send, note_recv,
):
    me, seq = lax.axis_index("grp"), lax.axis_index("seq")
    x_loads = started(*((x_hbm.at[j], x_buf.at[j], x_sem.at[j]) for j in range(CELLS)))
    loads = started(
        (pos_hbm, pos_ref, load_sem.at[0]), (count_hbm, count_ref, load_sem.at[1]),
        (norm_hbm, norm_ref, load_sem.at[2]), (qkv_hbm.at[0], qkv_ref, load_sem.at[3]),
    )

    hops = (0, 0, 1, 3, 1, 3, 2, 2)
    flips = (0, 1, 0, 0, 1, 1, 0, 1)

    def partner(i):
        return lax.rem(me // 2 + hops[i], CELLS // 2) * 2 + lax.rem(me + flips[i], 2)

    barrier = pltpu.get_barrier_semaphore()
    for i in range(1, CELLS):
        pl.semaphore_signal(barrier, inc=1, device_id=(partner(i), seq), device_id_type=MESH)
    finished(loads[:2])
    finished(x_loads)
    row = lax.broadcasted_iota(I32, (CELLS, CELL), 0)
    for owner in range(CELLS):
        index, place, count = jnp.int32(0), jnp.int32(0), jnp.int32(0)
        for j in range(CELLS):
            position = pos_ref[j]
            mine = position // CELLS == owner
            index = jnp.where(mine, j, index)
            place = jnp.where(mine, position % CELLS, place)
            count = jnp.where(mine, count_ref[j], count)
        out_buf[owner] = x_buf[index]
        note_out[owner] = jnp.where(row == 0, place, count)
    pl.semaphore_wait(barrier, CELLS - 1)

    def sent(i):
        owner = partner(i)
        return (
            pltpu.make_async_remote_copy(
                out_buf.at[owner], cells_ref.at[i], send.at[i], recv.at[i],
                device_id=(owner, seq), device_id_type=MESH),
            pltpu.make_async_remote_copy(
                note_out.at[owner], note_in.at[i], note_send.at[i], note_recv.at[i],
                device_id=(owner, seq), device_id_type=MESH),
        )

    copies = [sent(i) for i in range(1, CELLS)]
    for pair in copies:
        for copy in pair:
            copy.start()
    finished(loads[2:])
    turn(qkv_ref, w_ref)
    gain, offset = norm_ref[0, 0:1, :], norm_ref[0, 1:2, :]
    peak_ref[...] = jnp.zeros_like(peak_ref)

    def take(i):
        for pair in copies[max(i - 1, 0) : i + 1]:
            for copy in pair:
                copy.wait_recv()
        rows, valid = cells_in(
            jnp.concatenate([cells_ref[i], cells_ref[i + 1]], axis=0),
            [note_in[i, 1:2, 0:1], note_in[i + 1, 1:2, 0:1]])
        project(
            rows, valid, gain, offset, w_ref[...], qkv_ref[:, C : 2 * C],
            k_ref, v_ref, q_ref, peak_ref, i * CELL, i * CELL,
        )

    def pads(cells):
        return [(CELL - note_in[i, 1:2, 0:1]).astype(F32) for i in range(cells)]

    cells_ref[0] = out_buf[me]
    note_in[0] = note_out[me]
    part = (mixed_ref, total_ref)
    take(0)
    take(2)
    attend(EARLY, pads(4), k_ref, v_ref, q_ref, None, part, False, 1, 8)
    take(4)
    attend(LATER, pads(6), k_ref, v_ref, q_ref, None, part, False, 1, 8)
    take(6)
    lane = lax.broadcasted_iota(I32, (CELLS, CELL), 1)
    meta = jnp.zeros((CELLS, CELL), I32)
    for j in range(CELLS):
        meta = jnp.where(lane == j, note_in[j], meta)
    meta_ref[...] = meta
    widest(peak_ref)
    for pair in copies:
        for copy in pair:
            copy.wait_send()


def vmem():
    return pl.BlockSpec(memory_space=pltpu.VMEM)


def hbm():
    return pl.BlockSpec(memory_space=pltpu.HBM)


def shape(dims, dtype=BF16):
    return jax.ShapeDtypeStruct(dims, dtype)


def dma(*dims):
    return pltpu.SemaphoreType.DMA(dims)


def gather_cells(pos, counts, cells, norms, qkv):
    return pl.pallas_call(
        gather_kernel,
        out_shape=(
            shape((CELLS, CELL, C)), shape((ROWS, C)), shape((C, ROWS)), shape((C, ROWS)),
            shape((CELLS, CELL), I32), shape((CELLS, CELL), F32), shape((C, HALF), F32), shape((HEADS, HALF), F32),
        ),
        in_specs=[hbm()] * 5,
        out_specs=(vmem(),) * 8,
        scratch_shapes=[
            pltpu.SMEM((CELLS,), I32),
            pltpu.SMEM((CELLS,), I32),
            pltpu.VMEM((CELLS, CELL, C), BF16),
            pltpu.VMEM((2, 4, C), F32),
            pltpu.VMEM((CELLS, CELL, C), BF16),
            pltpu.VMEM((CELLS, CELLS, CELL), I32),
            pltpu.VMEM((CELLS, CELLS, CELL), I32),
            pltpu.VMEM((C, 3 * C), BF16),
            pltpu.VMEM((2 * C, C), BF16),
            dma(4), dma(CELLS), dma(CELLS), dma(CELLS), dma(CELLS), dma(CELLS),
        ],
        compiler_params=pltpu.CompilerParams(
            collective_id=0, has_side_effects=True, vmem_limit_bytes=32 * 2**20),
        name="gather_cells",
    )(pos, counts, cells, norms, qkv)


def aligned_kernel(
    meta_ref, peak_ref, k_ref, v_ref, q_ref, cells_ref, mixed_ref, total_ref, m_ref, placed_ref, count_ref,
    place_ref, mix_ref, sem,
):
    loads = started((meta_ref, place_ref, sem.at[0]))
    pads = [(CELL - meta_ref[1:2, j : j + 1]).astype(F32) for j in range(CELLS)]
    attend_any(((LAST, 1, 8), (OTHERS, 8, 1)), ALIGNED, None, pads, peak_ref, k_ref, v_ref, q_ref, mix_ref, (mixed_ref, total_ref))
    finished(loads)
    for j in range(CELLS):
        to = place_ref[0, j]
        m_ref[:, pl.ds(pl.multiple_of(to * CELL, CELL), CELL)] = mix_ref[:, j * CELL : (j + 1) * CELL]
        placed_ref[to] = cells_ref[j]
        count_ref[pl.ds(to, 1), :] = jnp.full((1, CELL), place_ref[1, j], I32)


def aligned_attention(meta, peak, keys, values, queries, cells, mixed, total):
    return pl.pallas_call(
        aligned_kernel,
        out_shape=(shape((C, ROWS)), shape((CELLS, CELL, C)), shape((CELLS, CELL), I32)),
        in_specs=[vmem()] * 8,
        out_specs=(vmem(),) * 3,
        scratch_shapes=[
            pltpu.SMEM((CELLS, CELL), I32),
            pltpu.VMEM((C, ROWS), BF16),
            dma(1),
        ],
        compiler_params=pltpu.CompilerParams(vmem_limit_bytes=36 * 2**20),
        name="aligned_attention",
    )(meta, peak, keys, values, queries, cells, mixed, total)


def along(step):
    n_grp, n_seq = lax.axis_size("grp"), lax.axis_size("seq")
    flat = lax.axis_index("grp") * n_seq + lax.axis_index("seq")
    other = lax.rem(flat + step + n_grp * n_seq, n_grp * n_seq)
    return (other // n_seq, lax.rem(other, n_seq))


def middle_kernel(
    note_ref, x_ref, m_ref, norm_ref, qkv_ref, out_ref, up_ref, down_ref,
    y_ref, k_ref, v_ref, q_ref, all_count_ref, peak_ref, mixed_ref, total_ref,
    before_ref, after_ref, note_before, note_after, w_ref, ready,
    send_before, send_after, recv_before, recv_after, note_send, note_recv,
):
    after, before = along(1), along(-1)
    barrier = pltpu.get_barrier_semaphore()
    pl.semaphore_signal(barrier, inc=1, device_id=before, device_id_type=MESH)
    turn(qkv_ref.at[1], w_ref)
    gain, offset = norm_ref[1, 0:1, :], norm_ref[1, 1:2, :]
    peak_ref[...] = jnp.zeros_like(peak_ref)
    notes = [
        pltpu.make_async_remote_copy(
            note_ref, target, note_send.at[i], note_recv.at[i], device_id=device, device_id_type=MESH)
        for i, (target, device) in enumerate(((note_after, before), (note_before, after)))
    ]

    def to_before(i):
        return pltpu.make_async_remote_copy(
            y_ref.at[pl.ds(i * STEP, STEP)], after_ref.at[pl.ds(i * STEP, STEP)],
            send_before.at[i], recv_after.at[i], device_id=before, device_id_type=MESH)

    def to_after(i):
        return pltpu.make_async_remote_copy(
            y_ref.at[pl.ds(HALF + i * STEP, STEP)], before_ref.at[pl.ds(i * STEP, STEP)],
            send_after.at[i], recv_before.at[i], device_id=after, device_id_type=MESH)

    def place(rows, counts, k_at, q_at):
        rows, valid = cells_in(rows, counts)
        project(
            rows, valid, gain, offset, w_ref[...], qkv_ref[1, :, C : 2 * C],
            k_ref, v_ref, q_ref, peak_ref, k_at, q_at,
        )

    for chunk in (2, 3, 0, 1):
        at = chunk * STEP
        y_ref[at : at + STEP, :] = finish(
            jnp.concatenate([x_ref[2 * chunk], x_ref[2 * chunk + 1]], axis=0), m_ref[:, at : at + STEP],
            norm_ref[0, 2:3, :], norm_ref[0, 3:4, :], out_ref[0], up_ref[0], down_ref[0],
        )
        if chunk == 3:
            pl.semaphore_wait(barrier, 1)
            pl.semaphore_signal(ready, inc=1, device_id=after, device_id_type=MESH)
            notes[1].start()
            to_after(0).start()
    to_after(1).start()
    own = [note_ref[p : p + 1, 0:1] for p in range(CELLS)]
    place(y_ref[HALF:, :], own[4:], ROWS, HALF)
    place(y_ref[:HALF, :], own[:4], HALF, 0)
    pl.semaphore_wait(ready, 1)
    for copy in (notes[0], to_before(0), to_before(1)):
        copy.start()
    part = (mixed_ref, total_ref)
    pads = [None] * 4 + [(CELL - count).astype(F32) for count in own]
    attend(OWN, pads, k_ref, v_ref, q_ref, None, part, False, 1, 8)
    for copy in notes:
        copy.wait()
    before_counts = [note_before[p : p + 1, 0:1] for p in range(4, 8)]
    after_counts = [note_after[p : p + 1, 0:1] for p in range(4)]
    pads = [(CELL - count).astype(F32) for count in before_counts + own + after_counts]
    for i in range(2):
        to_before(i).wait_recv()
    place(after_ref[...], after_counts, HALF + ROWS, None)
    attend(AFTER, pads, k_ref, v_ref, q_ref, None, part, False, 1, 8)
    to_after(0).wait_recv()
    place(before_ref[:STEP, :], before_counts[:2], 0, None)
    attend(BEFORE, pads, k_ref, v_ref, q_ref, None, part, False, 1, 8)
    to_after(1).wait_recv()
    place(before_ref[STEP:, :], before_counts[2:], STEP, None)
    all_count_ref[0:4, :] = note_before[4:8, :]
    all_count_ref[4:12, :] = note_ref[...]
    all_count_ref[12:16, :] = note_after[0:4, :]
    widest(peak_ref)
    for i in range(2):
        to_before(i).wait_send()
        to_after(i).wait_send()


def middle(notes, cells, mixture, norms, qkv, out_w, up_w, down_w):
    return pl.pallas_call(
        middle_kernel,
        out_shape=(
            shape((ROWS, C)), shape((2 * ROWS, C)), shape((C, 2 * ROWS)), shape((C, ROWS)),
            shape((2 * CELLS, CELL), I32), shape((CELLS, CELL), F32), shape((C, ROWS), F32), shape((HEADS, ROWS), F32),
        ),
        in_specs=[vmem()] * 8,
        out_specs=(vmem(),) * 8,
        scratch_shapes=[
            pltpu.VMEM((HALF, C), BF16),
            pltpu.VMEM((HALF, C), BF16),
            pltpu.VMEM((CELLS, CELL), I32),
            pltpu.VMEM((CELLS, CELL), I32),
            pltpu.VMEM((2 * C, C), BF16),
            pltpu.SemaphoreType.REGULAR,
            dma(2), dma(2), dma(2), dma(2), dma(2), dma(2),
        ],
        compiler_params=pltpu.CompilerParams(
            collective_id=1, has_side_effects=True, vmem_limit_bytes=32 * 2**20),
        name="middle",
    )(notes, cells, mixture, norms, qkv, out_w, up_w, down_w)


def shifted_kernel(
    count_ref, peak_ref, k_ref, v_ref, q_ref, mixed_ref, total_ref, x_ref, norm_ref, out_ref, up_ref, down_ref,
    y_hbm, m_ref, y_ref, store_sem,
):
    pads = [(CELL - count_ref[j : j + 1, 0:1]).astype(F32) for j in range(2 * CELLS)]
    attend_any(((BORROWED, 1, 8),), SHIFTED, HALF, pads, peak_ref, k_ref, v_ref, q_ref, m_ref, (mixed_ref, total_ref))
    stores = []
    for i in range(ROWS // HALF):
        at = i * HALF
        done = finish(
            x_ref[at : at + HALF, :], m_ref[:, at : at + HALF], norm_ref[1, 2:3, :], norm_ref[1, 3:4, :],
            out_ref[1], up_ref[1], down_ref[1],
        )
        for u in range(4):
            cell = CELLS // 2 + 4 * i + u
            keep = lax.broadcasted_iota(I32, (CELL, 1), 0) < count_ref[cell : cell + 1, 0:1]
            part = done[u * CELL : (u + 1) * CELL, :]
            y_ref[at + u * CELL : at + (u + 1) * CELL, :] = jnp.where(keep, part, jnp.zeros_like(part))
        rows = pl.ds(at, HALF)
        stores += started((y_ref.at[rows], y_hbm.at[rows], store_sem.at[i]))
    finished(stores)


def shifted_block(counts, peak, keys, values, queries, mixed, total, rows, norms, out_w, up_w, down_w):
    return pl.pallas_call(
        shifted_kernel,
        out_shape=shape((ROWS, C)),
        in_specs=[vmem()] * 12,
        out_specs=hbm(),
        scratch_shapes=[
            pltpu.VMEM((C, ROWS), BF16),
            pltpu.VMEM((ROWS, C), BF16),
            dma(4),
        ],
        compiler_params=pltpu.CompilerParams(vmem_limit_bytes=36 * 2**20),
        name="shifted_block",
    )(counts, peak, keys, values, queries, mixed, total, rows, norms, out_w, up_w, down_w)


def body(points, hilbert_pos, valid_counts, norms, qkv, out_w, up_w, down_w):
    cells, keys, values, queries, meta, peak, mixed, total = gather_cells(*(
        pltpu.with_memory_space_constraint(array, pltpu.HBM)
        for array in (hilbert_pos, valid_counts, points.reshape(CELLS, CELL, C), norms, qkv)))
    mixture, placed, notes = aligned_attention(meta, peak, keys, values, queries, cells, mixed, total)
    rows, keys, values, queries, counts, peak, mixed, total = middle(notes, placed, mixture, norms, qkv, out_w, up_w, down_w)
    return shifted_block(
        counts, peak, keys, values, queries, mixed, total, rows, norms, out_w, up_w, down_w)


def solution(mesh):
    return jax.shard_map(
        body,
        mesh=mesh,
        in_specs=(
            P(("grp", "seq"), None), P(("grp", "seq")), P(("grp", "seq")), P(), P(), P(), P(), P(),
        ),
        out_specs=P(("grp", "seq"), None),
        check_vma=False,
    )
```

```python
import math

import jax
import jax.numpy as jnp
from jax import lax
from jax.experimental import pallas as pl
from jax.experimental.pallas import tpu as pltpu
from jax.sharding import PartitionSpec as P

C = 256
HEADS = 16
HD = 16
HID = 1024
CELL = 128
CELLS = 8
ROWS = CELL * CELLS
HALF = ROWS // 2
STEP = 2 * CELL
F32 = jnp.float32
BF16 = jnp.bfloat16
I32 = jnp.int32
MESH = pl.DeviceIdType.MESH
SCORE_SCALE = HD**-0.5 * math.log2(math.e)
SAFE_EXPONENT = 60.0
SAFE_VALUE = 2.0**40
EARLY = ((0, HALF, 0, HALF, False, False),)
LATER = ((0, HALF, HALF, STEP, True, False),)
LAST = ((0, HALF, HALF + STEP, STEP, True, True),)
OTHERS = ((HALF, HALF, 0, ROWS, False, True),)
ALIGNED = ((0, HALF, 0, ROWS, False, True), (HALF, HALF, 0, ROWS, False, True))
OWN = ((0, HALF, HALF, HALF, False, False), (HALF, HALF, ROWS, HALF, False, False))
AFTER = ((HALF, HALF, ROWS + HALF, HALF, True, False),)
BEFORE = ((0, HALF, 0, STEP, True, False),)
BORROWED = ((0, HALF, STEP, STEP, True, True),)
SHIFTED = ((0, HALF, 0, ROWS, False, True), (HALF, HALF, ROWS, ROWS, False, True))


def nt_dot(a, b):
    return lax.dot_general(a, b, (((1,), (1,)), ((), ())), preferred_element_type=F32)


def nn_dot(a, b):
    return jnp.dot(a, b, preferred_element_type=F32)


def norm_rows_of(values, gain, offset):
    center = jnp.mean(values, axis=-1, keepdims=True)
    spread = values - center
    second = jnp.mean(spread * spread, axis=-1, keepdims=True)
    return spread * lax.rsqrt(second + 1e-5) * gain + offset


def head_pick(rows, columns, channel_axis):
    channel = lax.broadcasted_iota(I32, (rows, columns), channel_axis) // HD
    head = lax.broadcasted_iota(I32, (rows, columns), 1 - channel_axis)
    return jnp.where(channel == head, 1.0, 0.0).astype(BF16)


def first_valid(rows, count):
    index = lax.broadcasted_iota(I32, (CELL, 1), 0)
    return jnp.where(index < count, rows, rows[0:1, :])


def lane_valid(count):
    return jnp.where(lax.broadcasted_iota(I32, (1, CELL), 1) < count, 1.0, 0.0)


def raise_peak(peak_ref, row, tall):
    peak = peak_ref[row : row + 1, :]
    for at in range(0, tall.shape[1], CELL):
        peak = jnp.maximum(peak, tall[:, at : at + CELL])
    peak_ref[row : row + 1, :] = peak


def cells_in(rows, counts):
    wide = rows.astype(F32)
    cells = [first_valid(wide[u * CELL : (u + 1) * CELL], count) for u, count in enumerate(counts)]
    return jnp.concatenate(cells, axis=0), jnp.concatenate([lane_valid(count) for count in counts], axis=1)


def project(rows, valid, gain, offset, w_t, w_k, k_ref, v_ref, q_ref, peak_ref, k_at, q_at):
    count = rows.shape[0]
    normed = norm_rows_of(rows, gain, offset).astype(BF16)
    keys = nn_dot(normed, w_k).astype(BF16)
    k_ref[pl.ds(k_at, count), :] = keys
    values = nt_dot(w_t[C:, :], normed) * valid
    v_ref[:, pl.ds(k_at, count)] = values.astype(BF16)
    wide = keys.astype(F32)
    sums = nn_dot((wide * wide).astype(BF16), head_pick(C, CELL, 0))
    raise_peak(peak_ref, 0, jnp.max(sums, axis=0, keepdims=True))
    raise_peak(peak_ref, 2, jnp.max(jnp.abs(values), axis=0, keepdims=True))
    if q_at is not None:
        queries = nt_dot(w_t[:C, :], normed).astype(BF16)
        q_ref[:, pl.ds(q_at, count)] = queries
        wide = queries.astype(F32)
        sums = nn_dot(head_pick(HEADS, C, 1), (wide * wide).astype(BF16))
        raise_peak(peak_ref, 1, jnp.max(sums, axis=0, keepdims=True))


def turn(qkv_ref, w_ref):
    for at, source in ((0, 0), (C, 2 * C)):
        w_ref[at : at + C, :] = qkv_ref[:, source : source + C].astype(F32).T.astype(BF16)


def attend(windows, pads, k_ref, v_ref, q_ref, m_ref, part, exact, unroll, group, first=0, last=HEADS):
    def some_heads(first):
        rows = pl.ds(pl.multiple_of(first * HD, HD * group), HD * group)
        half = pl.ds(pl.multiple_of((first // 8) * CELL, CELL), CELL)
        for q_lo, q_n, k_lo, k_n, goes_on, ends in windows:
            q_at = pl.ds(q_lo, q_n)
            lane_head = lax.broadcasted_iota(I32, (CELL, q_n), 0) // HD
            queries = q_ref[half, q_at]
            queries = jnp.concatenate(
                [jnp.where(lane_head == (first + g) % 8, queries, jnp.zeros_like(queries)) for g in range(group)],
                axis=1)
            scores = nn_dot(k_ref[k_lo : k_lo + k_n, half], queries)
            if exact:
                scores = scores - jnp.max(scores, axis=0, keepdims=True)
            weights = jnp.exp2(scores * SCORE_SCALE)
            totals = jnp.sum(jnp.sum(weights.reshape(k_n // 8, 8, group * q_n), axis=0), axis=0, keepdims=True)
            for cell in range(k_n // CELL):
                totals = totals - pads[k_lo // CELL + cell] * weights[cell * CELL : cell * CELL + 1, :]
            mixes = nn_dot(v_ref[rows, k_lo : k_lo + k_n], weights.astype(BF16))
            for g in range(group):
                row = pl.ds(pl.multiple_of((first + g) * HD, HD), HD)
                mixed = mixes[g * HD : (g + 1) * HD, g * q_n : (g + 1) * q_n]
                total = totals[:, g * q_n : (g + 1) * q_n]
                if goes_on:
                    mixed = mixed + part[0][row, q_at]
                    total = total + part[1][pl.ds(first + g, 1), q_at]
                if ends:
                    m_ref[row, q_at] = (mixed / total).astype(BF16)
                else:
                    part[0][row, q_at] = mixed
                    part[1][pl.ds(first + g, 1), q_at] = total

    def step(i, carry):
        for u in range(unroll):
            some_heads((i * unroll + u) * group)
        return carry

    lax.fori_loop(first // (unroll * group), last // (unroll * group), step, 0)


def attend_any(plan, whole_windows, settled, pads, peak_ref, k_ref, v_ref, q_ref, m_ref, part):
    bound = peak_ref[0:1, :] * peak_ref[1:2, :] * SCORE_SCALE**2
    off = (bound >= SAFE_EXPONENT * SAFE_EXPONENT) | (peak_ref[2:3, :] >= SAFE_VALUE)
    safe = jnp.max(jnp.where(off, 1.0, 0.0)) < 0.5

    @pl.when(safe)
    def _():
        for windows, unroll, group in plan:
            attend(windows, pads, k_ref, v_ref, q_ref, m_ref, part, False, unroll, group)
        for head in range(HEADS if settled is not None else 0):
            row = slice(head * HD, (head + 1) * HD)
            m_ref[row, settled:] = (part[0][row, settled:] / part[1][head : head + 1, settled:]).astype(BF16)

    @pl.when(jnp.logical_not(safe))
    def _():
        attend(whole_windows, pads, k_ref, v_ref, q_ref, m_ref, part, True, 1, 1)


def gelu(values):
    return 0.5 * values * (1.0 + lax.erf(values * (2.0**-0.5)))


def finish(rows, mixture_t, gain, offset, out_w, up_w, down_w):
    residual = rows.astype(F32) + nn_dot(mixture_t.astype(F32).T.astype(BF16), out_w)
    residual = residual.astype(BF16).astype(F32)
    normed = norm_rows_of(residual, gain, offset).astype(BF16)
    hidden = gelu(nn_dot(normed, up_w)).astype(BF16)
    return (residual + nn_dot(hidden, down_w)).astype(BF16)


def widest(peak_ref):
    peak_ref[...] = jnp.broadcast_to(jnp.max(peak_ref[...], axis=1, keepdims=True), peak_ref.shape)


def started(*pairs):
    copies = [pltpu.make_async_copy(*pair) for pair in pairs]
    for copy in copies:
        copy.start()
    return copies


def finished(copies):
    for copy in copies:
        copy.wait()


def gather_kernel(
    pos_hbm, count_hbm, x_hbm, norm_hbm, qkv_hbm,
    cells_ref, k_ref, v_ref, q_ref, meta_ref, peak_ref, mixed_ref, total_ref,
    pos_ref, count_ref, x_buf, norm_ref, out_buf, note_out, note_in, qkv_ref, w_ref,
    load_sem, x_sem, send, recv, note_send, note_recv,
):
    me, seq = lax.axis_index("grp"), lax.axis_index("seq")
    x_loads = started(*((x_hbm.at[j], x_buf.at[j], x_sem.at[j]) for j in range(CELLS)))
    loads = started(
        (pos_hbm, pos_ref, load_sem.at[0]), (count_hbm, count_ref, load_sem.at[1]),
        (norm_hbm, norm_ref, load_sem.at[2]), (qkv_hbm.at[0], qkv_ref, load_sem.at[3]),
    )

    hops = (0, 0, 1, 3, 1, 3, 2, 2)
    flips = (0, 1, 0, 0, 1, 1, 0, 1)

    def partner(i):
        return lax.rem(me // 2 + hops[i], CELLS // 2) * 2 + lax.rem(me + flips[i], 2)

    barrier = pltpu.get_barrier_semaphore()
    for i in range(1, CELLS):
        pl.semaphore_signal(barrier, inc=1, device_id=(partner(i), seq), device_id_type=MESH)
    finished(loads[:2])
    finished(x_loads)
    row = lax.broadcasted_iota(I32, (CELLS, CELL), 0)
    for owner in range(CELLS):
        index, place, count = jnp.int32(0), jnp.int32(0), jnp.int32(0)
        for j in range(CELLS):
            position = pos_ref[j]
            mine = position // CELLS == owner
            index = jnp.where(mine, j, index)
            place = jnp.where(mine, position % CELLS, place)
            count = jnp.where(mine, count_ref[j], count)
        out_buf[owner] = x_buf[index]
        note_out[owner] = jnp.where(row == 0, place, count)
    pl.semaphore_wait(barrier, CELLS - 1)

    def sent(i):
        owner = partner(i)
        return (
            pltpu.make_async_remote_copy(
                out_buf.at[owner], cells_ref.at[i], send.at[i], recv.at[i],
                device_id=(owner, seq), device_id_type=MESH),
            pltpu.make_async_remote_copy(
                note_out.at[owner], note_in.at[i], note_send.at[i], note_recv.at[i],
                device_id=(owner, seq), device_id_type=MESH),
        )

    copies = [sent(i) for i in range(1, CELLS)]
    for pair in copies:
        for copy in pair:
            copy.start()
    finished(loads[2:])
    turn(qkv_ref, w_ref)
    gain, offset = norm_ref[0, 0:1, :], norm_ref[0, 1:2, :]
    peak_ref[...] = jnp.zeros_like(peak_ref)

    def take(i):
        for pair in copies[max(i - 1, 0) : i + 1]:
            for copy in pair:
                copy.wait_recv()
        rows, valid = cells_in(
            jnp.concatenate([cells_ref[i], cells_ref[i + 1]], axis=0),
            [note_in[i, 1:2, 0:1], note_in[i + 1, 1:2, 0:1]])
        project(
            rows, valid, gain, offset, w_ref[...], qkv_ref[:, C : 2 * C],
            k_ref, v_ref, q_ref, peak_ref, i * CELL, i * CELL,
        )

    def pads(cells):
        return [(CELL - note_in[i, 1:2, 0:1]).astype(F32) for i in range(cells)]

    cells_ref[0] = out_buf[me]
    note_in[0] = note_out[me]
    part = (mixed_ref, total_ref)
    take(0)
    take(2)
    attend(EARLY, pads(4), k_ref, v_ref, q_ref, None, part, False, 1, 8)
    take(4)
    attend(LATER, pads(6), k_ref, v_ref, q_ref, None, part, False, 1, 8)
    take(6)
    lane = lax.broadcasted_iota(I32, (CELLS, CELL), 1)
    meta = jnp.zeros((CELLS, CELL), I32)
    for j in range(CELLS):
        meta = jnp.where(lane == j, note_in[j], meta)
    meta_ref[...] = meta
    widest(peak_ref)
    for pair in copies:
        for copy in pair:
            copy.wait_send()


def vmem():
    return pl.BlockSpec(memory_space=pltpu.VMEM)


def hbm():
    return pl.BlockSpec(memory_space=pltpu.HBM)


def shape(dims, dtype=BF16):
    return jax.ShapeDtypeStruct(dims, dtype)


def dma(*dims):
    return pltpu.SemaphoreType.DMA(dims)


def gather_cells(pos, counts, cells, norms, qkv):
    return pl.pallas_call(
        gather_kernel,
        out_shape=(
            shape((CELLS, CELL, C)), shape((ROWS, C)), shape((C, ROWS)), shape((C, ROWS)),
            shape((CELLS, CELL), I32), shape((CELLS, CELL), F32), shape((C, HALF), F32), shape((HEADS, HALF), F32),
        ),
        in_specs=[hbm()] * 5,
        out_specs=(vmem(),) * 8,
        scratch_shapes=[
            pltpu.SMEM((CELLS,), I32),
            pltpu.SMEM((CELLS,), I32),
            pltpu.VMEM((CELLS, CELL, C), BF16),
            pltpu.VMEM((2, 4, C), F32),
            pltpu.VMEM((CELLS, CELL, C), BF16),
            pltpu.VMEM((CELLS, CELLS, CELL), I32),
            pltpu.VMEM((CELLS, CELLS, CELL), I32),
            pltpu.VMEM((C, 3 * C), BF16),
            pltpu.VMEM((2 * C, C), BF16),
            dma(4), dma(CELLS), dma(CELLS), dma(CELLS), dma(CELLS), dma(CELLS),
        ],
        compiler_params=pltpu.CompilerParams(
            collective_id=0, has_side_effects=True, vmem_limit_bytes=32 * 2**20),
        name="gather_cells",
    )(pos, counts, cells, norms, qkv)


def aligned_kernel(
    meta_ref, peak_ref, k_ref, v_ref, q_ref, cells_ref, mixed_ref, total_ref, m_ref, placed_ref, count_ref,
    place_ref, mix_ref, sem,
):
    loads = started((meta_ref, place_ref, sem.at[0]))
    pads = [(CELL - meta_ref[1:2, j : j + 1]).astype(F32) for j in range(CELLS)]
    attend_any(((LAST, 1, 8), (OTHERS, 8, 1)), ALIGNED, None, pads, peak_ref, k_ref, v_ref, q_ref, mix_ref, (mixed_ref, total_ref))
    finished(loads)
    for j in range(CELLS):
        to = place_ref[0, j]
        m_ref[:, pl.ds(pl.multiple_of(to * CELL, CELL), CELL)] = mix_ref[:, j * CELL : (j + 1) * CELL]
        placed_ref[to] = cells_ref[j]
        count_ref[pl.ds(to, 1), :] = jnp.full((1, CELL), place_ref[1, j], I32)


def aligned_attention(meta, peak, keys, values, queries, cells, mixed, total):
    return pl.pallas_call(
        aligned_kernel,
        out_shape=(shape((C, ROWS)), shape((CELLS, CELL, C)), shape((CELLS, CELL), I32)),
        in_specs=[vmem()] * 8,
        out_specs=(vmem(),) * 3,
        scratch_shapes=[
            pltpu.SMEM((CELLS, CELL), I32),
            pltpu.VMEM((C, ROWS), BF16),
            dma(1),
        ],
        compiler_params=pltpu.CompilerParams(vmem_limit_bytes=36 * 2**20),
        name="aligned_attention",
    )(meta, peak, keys, values, queries, cells, mixed, total)


def along(step):
    n_grp, n_seq = lax.axis_size("grp"), lax.axis_size("seq")
    flat = lax.axis_index("grp") * n_seq + lax.axis_index("seq")
    other = lax.rem(flat + step + n_grp * n_seq, n_grp * n_seq)
    return (other // n_seq, lax.rem(other, n_seq))


def middle_kernel(
    note_ref, x_ref, m_ref, norm_ref, qkv_ref, out_ref, up_ref, down_ref,
    y_ref, k_ref, v_ref, q_ref, all_count_ref, peak_ref, mixed_ref, total_ref,
    before_ref, after_ref, note_before, note_after, w_ref, ready,
    send_before, send_after, recv_before, recv_after, note_send, note_recv,
):
    after, before = along(1), along(-1)
    barrier = pltpu.get_barrier_semaphore()
    pl.semaphore_signal(barrier, inc=1, device_id=before, device_id_type=MESH)
    turn(qkv_ref.at[1], w_ref)
    gain, offset = norm_ref[1, 0:1, :], norm_ref[1, 1:2, :]
    peak_ref[...] = jnp.zeros_like(peak_ref)
    notes = [
        pltpu.make_async_remote_copy(
            note_ref, target, note_send.at[i], note_recv.at[i], device_id=device, device_id_type=MESH)
        for i, (target, device) in enumerate(((note_after, before), (note_before, after)))
    ]

    def to_before(i):
        return pltpu.make_async_remote_copy(
            y_ref.at[pl.ds(i * STEP, STEP)], after_ref.at[pl.ds(i * STEP, STEP)],
            send_before.at[i], recv_after.at[i], device_id=before, device_id_type=MESH)

    def to_after(i):
        return pltpu.make_async_remote_copy(
            y_ref.at[pl.ds(HALF + i * STEP, STEP)], before_ref.at[pl.ds(i * STEP, STEP)],
            send_after.at[i], recv_before.at[i], device_id=after, device_id_type=MESH)

    def place(rows, counts, k_at, q_at):
        rows, valid = cells_in(rows, counts)
        project(
            rows, valid, gain, offset, w_ref[...], qkv_ref[1, :, C : 2 * C],
            k_ref, v_ref, q_ref, peak_ref, k_at, q_at,
        )

    for chunk in (2, 3, 0, 1):
        at = chunk * STEP
        y_ref[at : at + STEP, :] = finish(
            jnp.concatenate([x_ref[2 * chunk], x_ref[2 * chunk + 1]], axis=0), m_ref[:, at : at + STEP],
            norm_ref[0, 2:3, :], norm_ref[0, 3:4, :], out_ref[0], up_ref[0], down_ref[0],
        )
        if chunk == 2:
            pl.semaphore_wait(barrier, 1)
            pl.semaphore_signal(ready, inc=1, device_id=after, device_id_type=MESH)
            notes[1].start()
        if chunk == 3:
            to_after(0).start()
    to_after(1).start()
    own = [note_ref[p : p + 1, 0:1] for p in range(CELLS)]
    place(y_ref[HALF:, :], own[4:], ROWS, HALF)
    place(y_ref[:HALF, :], own[:4], HALF, 0)
    part = (mixed_ref, total_ref)
    pads = [None] * 4 + [(CELL - count).astype(F32) for count in own]
    attend(OWN[:1], pads, k_ref, v_ref, q_ref, None, part, False, 1, 8, 0, 8)
    pl.semaphore_wait(ready, 1)
    for copy in (notes[0], to_before(0), to_before(1)):
        copy.start()
    attend(OWN[:1], pads, k_ref, v_ref, q_ref, None, part, False, 1, 8, 8, HEADS)
    attend(OWN[1:], pads, k_ref, v_ref, q_ref, None, part, False, 1, 8)
    for copy in notes:
        copy.wait()
    before_counts = [note_before[p : p + 1, 0:1] for p in range(4, 8)]
    after_counts = [note_after[p : p + 1, 0:1] for p in range(4)]
    pads = [(CELL - count).astype(F32) for count in before_counts + own + after_counts]
    to_after(0).wait_recv()
    place(before_ref[:STEP, :], before_counts[:2], 0, None)
    attend(BEFORE, pads, k_ref, v_ref, q_ref, None, part, False, 1, 8)
    for i in range(2):
        to_before(i).wait_recv()
    place(after_ref[...], after_counts, HALF + ROWS, None)
    attend(AFTER, pads, k_ref, v_ref, q_ref, None, part, False, 1, 8)
    to_after(1).wait_recv()
    place(before_ref[STEP:, :], before_counts[2:], STEP, None)
    all_count_ref[0:4, :] = note_before[4:8, :]
    all_count_ref[4:12, :] = note_ref[...]
    all_count_ref[12:16, :] = note_after[0:4, :]
    widest(peak_ref)
    for i in range(2):
        to_before(i).wait_send()
        to_after(i).wait_send()


def middle(notes, cells, mixture, norms, qkv, out_w, up_w, down_w):
    return pl.pallas_call(
        middle_kernel,
        out_shape=(
            shape((ROWS, C)), shape((2 * ROWS, C)), shape((C, 2 * ROWS)), shape((C, ROWS)),
            shape((2 * CELLS, CELL), I32), shape((CELLS, CELL), F32), shape((C, ROWS), F32), shape((HEADS, ROWS), F32),
        ),
        in_specs=[vmem()] * 8,
        out_specs=(vmem(),) * 8,
        scratch_shapes=[
            pltpu.VMEM((HALF, C), BF16),
            pltpu.VMEM((HALF, C), BF16),
            pltpu.VMEM((CELLS, CELL), I32),
            pltpu.VMEM((CELLS, CELL), I32),
            pltpu.VMEM((2 * C, C), BF16),
            pltpu.SemaphoreType.REGULAR,
            dma(2), dma(2), dma(2), dma(2), dma(2), dma(2),
        ],
        compiler_params=pltpu.CompilerParams(
            collective_id=1, has_side_effects=True, vmem_limit_bytes=32 * 2**20),
        name="middle",
    )(notes, cells, mixture, norms, qkv, out_w, up_w, down_w)


def shifted_kernel(
    count_ref, peak_ref, k_ref, v_ref, q_ref, mixed_ref, total_ref, x_ref, norm_ref, out_ref, up_ref, down_ref,
    y_hbm, m_ref, y_ref, store_sem,
):
    pads = [(CELL - count_ref[j : j + 1, 0:1]).astype(F32) for j in range(2 * CELLS)]
    attend_any(((BORROWED, 1, 8),), SHIFTED, HALF, pads, peak_ref, k_ref, v_ref, q_ref, m_ref, (mixed_ref, total_ref))
    stores = []
    for i in range(ROWS // HALF):
        at = i * HALF
        done = finish(
            x_ref[at : at + HALF, :], m_ref[:, at : at + HALF], norm_ref[1, 2:3, :], norm_ref[1, 3:4, :],
            out_ref[1], up_ref[1], down_ref[1],
        )
        for u in range(4):
            cell = CELLS // 2 + 4 * i + u
            keep = lax.broadcasted_iota(I32, (CELL, 1), 0) < count_ref[cell : cell + 1, 0:1]
            part = done[u * CELL : (u + 1) * CELL, :]
            y_ref[at + u * CELL : at + (u + 1) * CELL, :] = jnp.where(keep, part, jnp.zeros_like(part))
        rows = pl.ds(at, HALF)
        stores += started((y_ref.at[rows], y_hbm.at[rows], store_sem.at[i]))
    finished(stores)


def shifted_block(counts, peak, keys, values, queries, mixed, total, rows, norms, out_w, up_w, down_w):
    return pl.pallas_call(
        shifted_kernel,
        out_shape=shape((ROWS, C)),
        in_specs=[vmem()] * 12,
        out_specs=hbm(),
        scratch_shapes=[
            pltpu.VMEM((C, ROWS), BF16),
            pltpu.VMEM((ROWS, C), BF16),
            dma(4),
        ],
        compiler_params=pltpu.CompilerParams(vmem_limit_bytes=36 * 2**20),
        name="shifted_block",
    )(counts, peak, keys, values, queries, mixed, total, rows, norms, out_w, up_w, down_w)


def body(points, hilbert_pos, valid_counts, norms, qkv, out_w, up_w, down_w):
    cells, keys, values, queries, meta, peak, mixed, total = gather_cells(*(
        pltpu.with_memory_space_constraint(array, pltpu.HBM)
        for array in (hilbert_pos, valid_counts, points.reshape(CELLS, CELL, C), norms, qkv)))
    mixture, placed, notes = aligned_attention(meta, peak, keys, values, queries, cells, mixed, total)
    rows, keys, values, queries, counts, peak, mixed, total = middle(notes, placed, mixture, norms, qkv, out_w, up_w, down_w)
    return shifted_block(
        counts, peak, keys, values, queries, mixed, total, rows, norms, out_w, up_w, down_w)


def solution(mesh):
    return jax.shard_map(
        body,
        mesh=mesh,
        in_specs=(
            P(("grp", "seq"), None), P(("grp", "seq")), P(("grp", "seq")), P(), P(), P(), P(), P(),
        ),
        out_specs=P(("grp", "seq"), None),
        check_vma=False,
    )
```
